16 devices in a mesh: vp: 2 (over z), dp: 8 (over y, x, core).
Axes of the slice: x: 2, y: 2, z: 2, core: 2. Of those that a mesh axis runs over, the one named last changes fastest.
Arguments:
- hidden: bfloat16 [96, 512, 1024], P('dp')
- mask_pos: int32 [96, 77], P('dp')
- labels: int32 [96, 77], P('dp')
- w_trans: bfloat16 [1024, 1024], replicated
- b_trans: float32 [1024], replicated
- ln_gain: float32 [1024], replicated
- ln_bias: float32 [1024], replicated
- emb_table: bfloat16 [30592, 1024], P('vp')
- b_vocab: float32 [30592], P('vp')
Outputs:
- output 1: float32 [], replicated
- output 2: bfloat16 [96, 512, 1024], P('dp')
- output 3: float32 [1024, 1024], replicated
- output 4: float32 [1024], replicated
- output 5: float32 [1024], replicated
- output 6: float32 [1024], replicated
- output 7: float32 [30592, 1024], P('vp')
- output 8: float32 [30592], P('vp')
All inputs are finite; a program needn't handle non-finite values.
Results may differ from the reference program's by a relative error of at most 0.0107086.
Values sent between devices are 32-bit elements.
A program may use at most 1 GiB of HBM per device.

```python
import jax
import jax.numpy as jnp
from jax import lax

HIDDEN = 1024
VOCAB_PAD = 30592
VOCAB_REAL = 30522
SEQ_LEN = 512
N_MASKS = 77
BATCH_ALL = 96
SHARDS = 2
LOG_VOCAB = (VOCAB_REAL - 1).bit_length()
LN_EPS = 1e-5
PAD_BIAS = -1.0e9


def head_norm(pre_act, ln_gain, ln_bias):
    gelu_out = jax.nn.gelu(pre_act, approximate=False)
    row_mean = jnp.mean(gelu_out, axis=-1, keepdims=True)
    centered = gelu_out - row_mean
    row_var = jnp.mean(centered * centered, axis=-1, keepdims=True)
    return centered * lax.rsqrt(row_var + LN_EPS) * ln_gain + ln_bias


def setup_inputs(seed: int = 0) -> dict:
    sub_keys = jax.random.split(jax.random.key(seed), 12)
    hidden = jax.random.normal(sub_keys[0], (BATCH_ALL, SEQ_LEN, HIDDEN), jnp.float32).astype(jnp.bfloat16)

    def draw_row(row_key):
        return jax.random.permutation(row_key, SEQ_LEN)[:N_MASKS]

    mask_pos = jax.vmap(draw_row)(jax.random.split(sub_keys[1], BATCH_ALL)).astype(jnp.int32)
    label_exp = jax.random.randint(sub_keys[2], (BATCH_ALL, N_MASKS), 0, LOG_VOCAB + 1)
    label_top = jnp.minimum(jnp.left_shift(jnp.ones_like(label_exp), label_exp), VOCAB_REAL)
    labels = jax.random.randint(sub_keys[3], (BATCH_ALL, N_MASKS), 0, label_top)
    labels = labels.at[0, 0].set(VOCAB_REAL - 1).astype(jnp.int32)
    w_trans = (jax.random.normal(sub_keys[4], (HIDDEN, HIDDEN), jnp.float32) * HIDDEN ** -0.5).astype(jnp.bfloat16)
    b_trans = 0.5 * jax.random.normal(sub_keys[5], (HIDDEN,), jnp.float32)
    ln_gain = 1.0 + 0.3 * jax.random.normal(sub_keys[6], (HIDDEN,), jnp.float32)
    ln_bias = 0.3 * jax.random.normal(sub_keys[7], (HIDDEN,), jnp.float32)
    emb_table = (jax.random.normal(sub_keys[8], (VOCAB_PAD, HIDDEN), jnp.float32) * HIDDEN ** -0.5).astype(jnp.bfloat16)
    bias_slope = jax.random.uniform(sub_keys[9], (), jnp.float32, 0.3, 0.6)
    bias_noise = jax.random.normal(sub_keys[10], (VOCAB_PAD,), jnp.float32)
    vocab_ids = jnp.arange(VOCAB_PAD)
    b_vocab = 0.5 * bias_noise - bias_slope * jnp.log1p(vocab_ids.astype(jnp.float32))
    b_vocab = jnp.where(vocab_ids < VOCAB_REAL, b_vocab, PAD_BIAS).astype(jnp.float32)
    return {"hidden": hidden, "mask_pos": mask_pos, "labels": labels, "w_trans": w_trans, "b_trans": b_trans, "ln_gain": ln_gain, "ln_bias": ln_bias, "emb_table": emb_table, "b_vocab": b_vocab}


def reference(hidden, mask_pos, labels, w_trans, b_trans, ln_gain, ln_bias, emb_table, b_vocab):
    n_rows = hidden.shape[0]
    n_tokens = n_rows * N_MASKS
    shard_rows = VOCAB_PAD // SHARDS
    masked_h = jnp.take_along_axis(hidden, mask_pos[:, :, None], axis=1).reshape(n_tokens, HIDDEN)
    pre_act = jnp.dot(masked_h, w_trans, preferred_element_type=jnp.float32) + b_trans
    u_norm, head_vjp = jax.vjp(head_norm, pre_act, ln_gain, ln_bias)
    u_bf16 = u_norm.astype(jnp.bfloat16)
    flat_labels = labels.reshape(n_tokens)
    emb_blocks = emb_table.reshape(SHARDS, shard_rows, HIDDEN)
    bias_blocks = b_vocab.reshape(SHARDS, shard_rows)
    row_starts = jnp.arange(SHARDS) * shard_rows
    row_ids = jnp.arange(shard_rows)

    def block_logits(emb_block, bias_block):
        return jnp.dot(u_bf16, emb_block.T, preferred_element_type=jnp.float32) + bias_block

    def block_stats(block):
        emb_block, bias_block, row_start = block
        logits = block_logits(emb_block, bias_block)
        local_max = jnp.max(logits, axis=1)
        local_sum = jnp.sum(jnp.exp(logits - local_max[:, None]), axis=1)
        is_label = (flat_labels - row_start)[:, None] == row_ids[None, :]
        label_logit = jnp.sum(jnp.where(is_label, logits, 0.0), axis=1)
        return local_max, local_sum, label_logit

    block_max, block_sum, block_label = lax.map(block_stats, (emb_blocks, bias_blocks, row_starts))
    global_max = jnp.max(block_max, axis=0)
    log_norm = global_max + jnp.log(jnp.sum(block_sum * jnp.exp(block_max - global_max), axis=0))
    mlm_loss = jnp.mean(log_norm - jnp.sum(block_label, axis=0))

    def block_grads(block):
        emb_block, bias_block, row_start = block
        logits = block_logits(emb_block, bias_block)
        is_label = (flat_labels - row_start)[:, None] == row_ids[None, :]
        d_logits = (jnp.exp(logits - log_norm[:, None]) - is_label.astype(jnp.float32)) / n_tokens
        d_logits_bf = d_logits.astype(jnp.bfloat16)
        d_emb_block = jnp.dot(d_logits_bf.T, u_bf16, preferred_element_type=jnp.float32)
        du_part = jnp.dot(d_logits_bf, emb_block, preferred_element_type=jnp.float32).astype(jnp.bfloat16)
        return d_emb_block, jnp.sum(d_logits, axis=0), du_part

    d_emb_blocks, d_bias_blocks, du_parts = lax.map(block_grads, (emb_blocks, bias_blocks, row_starts))
    d_unorm = jnp.sum(du_parts.astype(jnp.float32), axis=0)
    d_pre, d_ln_gain, d_ln_bias = head_vjp(d_unorm)
    d_pre_bf = d_pre.astype(jnp.bfloat16)
    d_w_trans = jnp.dot(masked_h.T, d_pre_bf, preferred_element_type=jnp.float32)
    d_b_trans = jnp.sum(d_pre, axis=0)
    d_masked = jnp.dot(d_pre_bf, w_trans.T, preferred_element_type=jnp.float32).astype(jnp.bfloat16)
    row_index = jnp.arange(n_rows)[:, None]
    d_hidden = jnp.zeros_like(hidden).at[row_index, mask_pos].set(d_masked.reshape(n_rows, N_MASKS, HIDDEN))
    return (mlm_loss, d_hidden, d_w_trans, d_b_trans, d_ln_gain, d_ln_bias, d_emb_blocks.reshape(VOCAB_PAD, HIDDEN), d_bias_blocks.reshape(VOCAB_PAD))
```

```python
import functools
import math

import jax
import jax.numpy as jnp
from jax import lax
from jax.experimental import pallas as pl
from jax.experimental.pallas import tpu as pltpu
from jax.sharding import PartitionSpec as P


LN_EPS = 1e-5
F32 = jnp.float32
BF16 = jnp.bfloat16
NT = (((1,), (1,)), ((), ()))
LANES = 128
SUBLANES = 16
ROWS = 32
NEGATIVE = -1e30
OWN_V = 512
TILE_V = 768
TILE_T = 512
GATHERED_TILES = 1


def gelu_parts(a):
    cdf = 0.5 * (1.0 + lax.erf(a * math.sqrt(0.5)))
    return cdf, a * cdf


def normalised(g):
    centered = g - jnp.mean(g, axis=-1, keepdims=True)
    scale = lax.rsqrt(jnp.mean(centered * centered, axis=-1, keepdims=True) + LN_EPS)
    return centered * scale, scale


def row_loop(rows, step, body):
    def run(i, carry):
        body(pl.multiple_of(i * step, step))
        return carry

    lax.fori_loop(0, rows // step, run, 0)


def window_start(n_masks, c):
    return pl.multiple_of(n_masks * c // SUBLANES * SUBLANES, SUBLANES)


def head_kernel(n_masks, window, label_at, vp_ref, key_ref, hidden_ref, w_ref, b_ref, gain_ref, beta_ref, label_ref,
                z_ref, pre_ref, u_ref, sent_ref, z_acc, u_acc):
    c = pl.program_id(0)
    slots, seq_len = z_ref.shape[0], hidden_ref.shape[0]
    half = sent_ref.shape[0]

    @pl.when(c == 0)
    def _():
        z_acc[...] = jnp.zeros_like(z_acc)

    here = pl.ds(window_start(n_masks, c), window)
    ids = c * seq_len + lax.broadcasted_iota(jnp.int32, (window, seq_len), 1)
    pick = (key_ref[here, :] == ids).astype(F32).astype(BF16)
    z_acc[here, :] += jnp.dot(pick, hidden_ref[...], preferred_element_type=F32)

    @pl.when(c == pl.num_programs(0) - 1)
    def _():
        z_ref[...] = z_acc[...].astype(BF16)
        pre_ref[...] = jnp.dot(z_ref[...], w_ref[...], preferred_element_type=F32) + b_ref[...]

        def norm(r):
            at = pl.ds(r, ROWS)
            _, g = gelu_parts(pre_ref[at, :])
            xhat, _ = normalised(g)
            u = xhat * gain_ref[...] + beta_ref[...]
            u_acc[at, :] = u
            u_ref[at, :] = u.astype(BF16)

        row_loop(slots, ROWS, norm)
        sent_ref[...] = u_acc[pl.ds(pl.multiple_of(vp_ref[0] * half, SUBLANES), half), :]

        @pl.when(vp_ref[0] == label_at // half)
        def _():
            sent_ref[label_at % half : label_at % half + 1, :] = label_ref[...]


def head(vp, mask_pos, hidden, w, b, gain, beta, label_row, slots, half):
    n_rows, seq_len, width = hidden.shape
    n_masks = mask_pos.shape[1]
    key = (mask_pos + seq_len * jnp.arange(n_rows)[:, None]).reshape(-1, 1)
    key = jnp.pad(key, ((0, slots - n_rows * n_masks), (0, 0)), constant_values=-1)
    whole = lambda rows, cols: pl.BlockSpec((rows, cols), lambda c, v: (0, 0), pipeline_mode=pl.Buffered(1))
    out = lambda rows: pl.BlockSpec((rows, width), lambda c, v: (0, 0), pipeline_mode=pl.Buffered(1))
    return pl.pallas_call(
        functools.partial(head_kernel, n_masks, window_rows(n_masks), n_rows * n_masks),
        name="head",
        grid_spec=pltpu.PrefetchScalarGridSpec(
            num_scalar_prefetch=1,
            grid=(n_rows,),
            in_specs=[whole(slots, 1), pl.BlockSpec((None, seq_len, width), lambda c, v: (c, 0, 0)), whole(width, width)] + [whole(1, width)] * 4,
            out_specs=[out(slots), out(slots), out(slots), out(half)],
            scratch_shapes=[pltpu.VMEM((slots, width), F32), pltpu.VMEM((slots, width), F32)],
        ),
        out_shape=[
            jax.ShapeDtypeStruct((slots, width), BF16),
            jax.ShapeDtypeStruct((slots, width), F32),
            jax.ShapeDtypeStruct((slots, width), BF16),
            jax.ShapeDtypeStruct((half, width), F32),
        ],
        compiler_params=pltpu.CompilerParams(vmem_limit_bytes=50_000_000),
        cost_estimate=pl.CostEstimate(flops=2 * slots * width * width * 4, bytes_accessed=hidden.size * 2, transcendentals=slots * width),
    )(vp, key, hidden, w, b.reshape(1, width), gain.reshape(1, width), beta.reshape(1, width), label_row)


def row_blocks(rows):
    n = 4
    sixteenths = rows // SUBLANES
    sizes = [(sixteenths // n + (i < sixteenths % n)) * SUBLANES for i in range(n)]
    return [slice(sum(sizes[:i]), sum(sizes[: i + 1])) for i in range(n)]


def stats_kernel(emb_ref, bias_ref, u_ref, logit_ref, max_ref, sum_ref, m_acc, l_acc):
    i = pl.program_id(0)

    @pl.when(i == 0)
    def _():
        m_acc[...] = jnp.full_like(m_acc, NEGATIVE)
        l_acc[...] = jnp.zeros_like(l_acc)

    blocks = row_blocks(u_ref.shape[0])

    def logits(rows):
        logit_ref[rows, :] = lax.dot_general(u_ref[rows, :], emb_ref[...], NT, preferred_element_type=F32) + bias_ref[...]

    def stats(rows):
        tiles = [logit_ref[rows, LANES * j : LANES * (j + 1)] for j in range(logit_ref.shape[1] // LANES)]
        old = m_acc[rows, :]
        top = functools.reduce(jnp.maximum, tiles, old)
        l_acc[rows, :] = l_acc[rows, :] * jnp.exp(old - top) + sum(jnp.exp(x - top) for x in tiles)
        m_acc[rows, :] = top

    logits(blocks[0])
    for before, rows in zip(blocks, blocks[1:]):
        logits(rows)
        stats(before)
    stats(blocks[-1])

    @pl.when(i == pl.num_programs(0) - 1)
    def _():
        top = jnp.max(m_acc[...], axis=-1, keepdims=True)
        max_ref[...] = top
        sum_ref[...] = jnp.sum(l_acc[...] * jnp.exp(m_acc[...] - top), axis=-1, keepdims=True)


def tile_of_rows(shard_rows, width):
    last = shard_rows - OWN_V
    return pl.BlockSpec((pl.Element(OWN_V), pl.Element(width)), lambda i: (pl.multiple_of(jnp.minimum(i * OWN_V, last), SUBLANES), 0))


def in_tiles(row, fill):
    n = row.shape[0]
    full = n // OWN_V
    again = OWN_V - n % OWN_V
    last = jnp.concatenate([jnp.full((again,), fill, row.dtype), row[full * OWN_V :]])
    return jnp.concatenate([row[: full * OWN_V], last]).reshape(full + 1, 1, OWN_V)


def own_stats(u, emb, bias):
    slots, width = u.shape
    bias = in_tiles(bias, NEGATIVE)
    n = bias.shape[0]
    col = pl.BlockSpec((slots, 1), lambda i: (0, 0))
    return pl.pallas_call(
        stats_kernel,
        name="own_stats",
        grid=(n,),
        in_specs=[
            tile_of_rows(emb.shape[0], width),
            pl.BlockSpec((None, 1, OWN_V), lambda i: (i, 0, 0)),
            pl.BlockSpec((slots, width), lambda i: (0, 0), pipeline_mode=pl.Buffered(1)),
        ],
        out_specs=[pl.BlockSpec((slots, OWN_V), lambda i: (0, i)), col, col],
        out_shape=[jax.ShapeDtypeStruct((slots, n * OWN_V), F32)] + [jax.ShapeDtypeStruct((slots, 1), F32)] * 2,
        scratch_shapes=[pltpu.VMEM((slots, LANES), F32)] * 2,
        compiler_params=pltpu.CompilerParams(vmem_limit_bytes=50_000_000),
        cost_estimate=pl.CostEstimate(flops=2 * slots * n * OWN_V * width, bytes_accessed=slots * n * OWN_V * 4, transcendentals=slots * n * OWN_V),
    )(emb, bias, u)


def du_kernel(inv_n, spare, logit_ref, emb_ref, ids_ref, lse_ref, lab_ref, du_ref, lse_b, lab_b, hit_acc, acc):
    i = pl.program_id(0)
    blocks = row_blocks(lse_ref.shape[0])

    @pl.when(i == 0)
    def _():
        acc[...] = jnp.zeros_like(acc)
        hit_acc[...] = jnp.zeros_like(hit_acc)
        lse_b[...] = jnp.broadcast_to(lse_ref[...], lse_b.shape)
        lab_b[...] = jnp.broadcast_to(lab_ref[...], lab_b.shape)

    def grad(rows):
        parts = []
        hits = hit_acc[rows, :]
        for j in range(logit_ref.shape[1] // LANES):
            cols = slice(LANES * j, LANES * (j + 1))
            x = logit_ref[rows, cols]
            hit = ids_ref[:, cols] == lab_b[rows, :]
            hits = hits + jnp.where(hit, x, 0.0)
            parts.append((jnp.exp(x - lse_b[rows, :]) - jnp.where(hit, inv_n, 0.0)).astype(BF16))
        hit_acc[rows, :] = hits
        return jnp.concatenate(parts, axis=1)

    for rows in blocks:
        acc[rows, :] += jnp.dot(grad(rows), emb_ref[...], preferred_element_type=F32)

    @pl.when(i == pl.num_programs(0) - 1)
    def _():
        du_ref[...] = acc[...].astype(BF16).astype(F32)
        du_ref[spare : spare + 1, :LANES] = jnp.sum(hit_acc[...], axis=0, keepdims=True)


def own_du(logits, emb, lse, labels, inv_n, n_own):
    slots, width = lse.shape[0], emb.shape[1]
    ids = in_tiles(jnp.arange(emb.shape[0], dtype=jnp.int32), 2**30)
    n = ids.shape[0]
    col = pl.BlockSpec((slots, 1), lambda i: (0, 0), pipeline_mode=pl.Buffered(1))
    return pl.pallas_call(
        functools.partial(du_kernel, inv_n, n_own),
        name="own_du",
        grid=(n,),
        in_specs=[
            pl.BlockSpec((slots, OWN_V), lambda i: (0, i)),
            tile_of_rows(emb.shape[0], width),
            pl.BlockSpec((None, 1, OWN_V), lambda i: (i, 0, 0)),
            col,
            col,
        ],
        out_specs=pl.BlockSpec((slots, width), lambda i: (0, 0), pipeline_mode=pl.Buffered(1)),
        out_shape=jax.ShapeDtypeStruct((slots, width), F32),
        scratch_shapes=[pltpu.VMEM((slots, LANES), F32), pltpu.VMEM((slots, LANES), jnp.int32), pltpu.VMEM((slots, LANES), F32), pltpu.VMEM((slots, width), F32)],
        compiler_params=pltpu.CompilerParams(vmem_limit_bytes=50_000_000),
        cost_estimate=pl.CostEstimate(flops=2 * slots * n * OWN_V * width, bytes_accessed=slots * n * OWN_V * 4, transcendentals=slots * n * OWN_V),
    )(logits, emb, ids, lse, labels)


def head_grad_kernel(n_own, n_tokens, du0_ref, du1_ref, pre_ref, z_ref, w_ref, gain_ref, lse_ref, sums_ref, dz_ref, dab_ref, b_acc, g_acc, o_acc):
    slots, width = pre_ref.shape
    for a in (b_acc, g_acc, o_acc):
        a[...] = jnp.zeros_like(a)

    def fold(x):
        return functools.reduce(jnp.add, [x[8 * j : 8 * (j + 1), :] for j in range(ROWS // 8)])

    def body(r):
        at = pl.ds(r, ROWS)
        real = r + lax.broadcasted_iota(jnp.int32, (ROWS, width), 0) < n_own
        du = jnp.where(real, du0_ref[at, :] + du1_ref[at, :], 0.0)
        a = pre_ref[at, :]
        cdf, g = gelu_parts(a)
        xhat, scale = normalised(g)
        dx = du * gain_ref[...]
        mean_dx = jnp.mean(dx, axis=-1, keepdims=True)
        mean_dxx = jnp.mean(dx * xhat, axis=-1, keepdims=True)
        dg = scale * (dx - mean_dx - xhat * mean_dxx)
        da = dg * (cdf + a * (math.sqrt(0.5 / math.pi) * jnp.exp(-0.5 * a * a)))
        b_acc[...] += fold(da)
        g_acc[...] += fold(du * xhat)
        o_acc[...] += fold(du)
        dab_ref[at, :] = da.astype(BF16)

    row_loop(slots, ROWS, body)
    sums_ref[:width, :] = lax.dot_general(z_ref[...], dab_ref[...], (((0,), (0,)), ((), ())), preferred_element_type=F32)
    dz_ref[...] = lax.dot_general(dab_ref[...], w_ref[...], NT, preferred_element_type=F32).astype(BF16)
    real = lax.broadcasted_iota(jnp.int32, (slots, 1), 0) < n_own
    norms = jnp.sum(jnp.where(real, lse_ref[...], 0.0))
    target = jnp.sum(du0_ref[n_own : n_own + 1, :LANES] + du1_ref[n_own : n_own + 1, :LANES])
    rows = lax.broadcasted_iota(jnp.int32, (8, width), 0)
    tail = jnp.where(rows == 3, (norms - target) / n_tokens, 0.0)
    for j, a in enumerate((b_acc, g_acc, o_acc)):
        tail = jnp.where(rows == j, jnp.sum(a[...], axis=0, keepdims=True), tail)
    sums_ref[width:, :] = tail


def head_grad(du0, du1, pre, z, w, gain, lse, n_own, n_tokens):
    slots, width = pre.shape
    vmem = pl.BlockSpec(memory_space=pltpu.VMEM)
    return pl.pallas_call(
        functools.partial(head_grad_kernel, n_own, n_tokens),
        name="head_grad",
        in_specs=[vmem] * 7,
        out_specs=[vmem] * 2,
        out_shape=[jax.ShapeDtypeStruct((width + 8, width), F32), jax.ShapeDtypeStruct((slots, width), BF16)],
        scratch_shapes=[pltpu.VMEM((slots, width), BF16)] + [pltpu.VMEM((8, width), F32)] * 3,
        compiler_params=pltpu.CompilerParams(vmem_limit_bytes=55_000_000),
        cost_estimate=pl.CostEstimate(flops=8 * slots * width * width, bytes_accessed=slots * width * 18, transcendentals=slots * width),
    )(du0, du1, pre, z, w, gain.reshape(1, width), lse)


def window_rows(n_masks):
    return -(-(n_masks + SUBLANES - 1) // SUBLANES) * SUBLANES


def scatter_kernel(n_masks, window, pos_ref, dz_ref, out_ref):
    c = pl.program_id(0)
    seq_len = out_ref.shape[0]
    hit = pos_ref[...] == lax.broadcasted_iota(jnp.int32, (seq_len, window), 0)
    rows = dz_ref[pl.ds(window_start(n_masks, c), window), :]
    out_ref[...] = jnp.dot(hit.astype(F32).astype(BF16), rows, preferred_element_type=F32).astype(BF16)


def scatter(mask_pos, dz, seq_len):
    n_rows, n_masks = mask_pos.shape
    width = dz.shape[1]
    window = window_rows(n_masks)
    lead = [n_masks * c % SUBLANES for c in range(n_rows)]
    pos = jnp.stack([jnp.pad(mask_pos[c], (a, window - n_masks - a), constant_values=-1) for c, a in enumerate(lead)])
    return pl.pallas_call(
        functools.partial(scatter_kernel, n_masks, window),
        name="scatter",
        grid=(n_rows,),
        in_specs=[pl.BlockSpec((None, 1, window), lambda c: (c, 0, 0)), pl.BlockSpec(dz.shape, lambda c: (0, 0), pipeline_mode=pl.Buffered(1))],
        out_specs=pl.BlockSpec((None, seq_len, width), lambda c: (c, 0, 0)),
        out_shape=jax.ShapeDtypeStruct((n_rows, seq_len, width), BF16),
        cost_estimate=pl.CostEstimate(flops=2 * n_rows * seq_len * window * width, bytes_accessed=n_rows * seq_len * width * 2, transcendentals=0),
    )(pos[:, None, :], dz)


def emb_grad_kernel(tc, n, tail, inv_n, bv, off_ref, lab_ref, lse_ref, emb_ref, bias_ref, u_ref, *rest):
    (*dout_refs, db_ref, s0, s1, bb_ref) = rest
    acc = dout_refs[0]
    row0 = (off_ref[0] + pl.program_id(0)) * bv
    bb_ref[...] = jnp.broadcast_to(bias_ref[...], (bv, LANES))
    db_ref[...] = jnp.zeros_like(db_ref)
    acc[...] = jnp.zeros_like(acc)

    def at(i):
        return i * tc if isinstance(i, int) else pl.multiple_of(i * tc, tc)

    def dot1(t0, w):
        return lax.dot_general(emb_ref[...], u_ref[pl.ds(t0, w), :], NT, preferred_element_type=F32)

    def grad(s_ref, t0, w):
        ids = row0 + lax.broadcasted_iota(jnp.int32, (bv, LANES), 0)
        total = None
        parts = []
        for j in range(w // LANES):
            cols = pl.ds(t0 + LANES * j, LANES)
            x = s_ref[:, LANES * j : LANES * (j + 1)] + bb_ref[...] - lse_ref[:, cols]
            g = jnp.exp(x) - jnp.where(ids == lab_ref[:, cols], inv_n, 0.0)
            total = g if total is None else total + g
            parts.append(g.astype(BF16))
        db_ref[...] += total
        return jnp.concatenate(parts, axis=1)

    def dot2(g, t0, w):
        acc[...] += jnp.dot(g, u_ref[pl.ds(t0, w), :], preferred_element_type=F32)

    s0[...] = dot1(0, tc)

    def body(i, carry):
        a = 2 * i
        s1[...] = dot1(at(a + 1), tc)
        dot2(grad(s0, at(a), tc), at(a), tc)
        s0[...] = dot1(at(a + 2), tc)
        dot2(grad(s1, at(a + 1), tc), at(a + 1), tc)
        return carry

    lax.fori_loop(0, n // 2 - 1, body, 0)
    s1[...] = dot1((n - 1) * tc, tc)
    dot2(grad(s0, (n - 2) * tc, tc), (n - 2) * tc, tc)
    if tail:
        s0[:, :tail] = dot1(n * tc, tail)
    dot2(grad(s1, (n - 1) * tc, tc), (n - 1) * tc, tc)
    if tail:
        dot2(grad(s0, n * tc, tail), n * tc, tail)
    for other in dout_refs[1:]:
        other[...] = acc[...]


def emb_grad(first_tile, n_tiles, place_rows, inv_n, labels, lse, emb, bias, u):
    n_tok, width = u.shape
    n, tail = divmod(n_tok, TILE_T)
    if n % 2:
        n, tail = n - 1, tail + TILE_T
    bv = TILE_V
    rows = n_tiles * bv
    once = pl.Buffered(1)
    out_specs = [pl.BlockSpec((bv, width), lambda i, o: (i, 0)), pl.BlockSpec((bv, LANES), lambda i, o: (i, 0))]
    out_shape = [jax.ShapeDtypeStruct((rows, width), F32), jax.ShapeDtypeStruct((rows, LANES), F32)]
    if place_rows:
        out_specs.insert(1, pl.BlockSpec((bv, width), lambda i, o: (o[0] + i, 0)))
        out_shape.insert(1, jax.ShapeDtypeStruct((place_rows, width), F32))
    grid_spec = pltpu.PrefetchScalarGridSpec(
        num_scalar_prefetch=1,
        grid=(n_tiles,),
        in_specs=[
            pl.BlockSpec((1, n_tok), lambda i, o: (0, 0), pipeline_mode=once),
            pl.BlockSpec((1, n_tok), lambda i, o: (0, 0), pipeline_mode=once),
            pl.BlockSpec((bv, width), lambda i, o: (o[0] + i, 0)),
            pl.BlockSpec((bv, 1), lambda i, o: (o[0] + i, 0)),
            pl.BlockSpec((n_tok, width), lambda i, o: (0, 0), pipeline_mode=once),
        ],
        out_specs=out_specs,
        scratch_shapes=[pltpu.VMEM((bv, TILE_T), F32), pltpu.VMEM((bv, TILE_T), F32), pltpu.VMEM((bv, LANES), F32)],
    )
    flops = 4 * rows * n_tok * width
    return pl.pallas_call(
        functools.partial(emb_grad_kernel, TILE_T, n, tail, inv_n, bv),
        grid_spec=grid_spec,
        out_shape=out_shape,
        compiler_params=pltpu.CompilerParams(vmem_limit_bytes=62_000_000),
        cost_estimate=pl.CostEstimate(flops=flops, bytes_accessed=n_tok * width * 2 + rows * width * 6, transcendentals=rows * n_tok),
    )(first_tile, labels, lse, emb, bias, u)


def round_kernel(src_ref, out_ref):
    out_ref[...] = src_ref[...].astype(out_ref.dtype)


def round_rows(src, block):
    rows, width = src.shape
    return pl.pallas_call(
        round_kernel,
        grid=(rows // block,),
        in_specs=[pl.BlockSpec((block, width), lambda i: (i, 0))],
        out_specs=pl.BlockSpec((block, width), lambda i: (i, 0)),
        out_shape=jax.ShapeDtypeStruct(src.shape, BF16),
        cost_estimate=pl.CostEstimate(flops=rows * width, bytes_accessed=rows * width * 6, transcendentals=0),
    )(src)


def copy_kernel(off_ref, src_ref, full_ref, out_ref):
    out_ref[...] = src_ref[...]


def put_rows(first_tile, src, full, n_src, n_tiles):
    bv, width = TILE_V, full.shape[1]
    return pl.pallas_call(
        copy_kernel,
        grid_spec=pltpu.PrefetchScalarGridSpec(
            num_scalar_prefetch=1,
            grid=(n_src, n_tiles),
            in_specs=[pl.BlockSpec((None, bv, width), lambda d, i, o: (d, i, 0)), pl.BlockSpec(memory_space=pl.ANY)],
            out_specs=pl.BlockSpec((bv, width), lambda d, i, o: (o[0] + d * n_tiles + i, 0)),
        ),
        out_shape=jax.ShapeDtypeStruct(full.shape, full.dtype),
        input_output_aliases={2: 0},
        cost_estimate=pl.CostEstimate(flops=n_src * n_tiles * bv * width, bytes_accessed=n_src * n_tiles * bv * width * 8, transcendentals=0),
    )(first_tile, src, full)


def solution(mesh):
    n_groups, n_vp = mesh.shape["dp"], mesh.shape["vp"]

    def local_step(hidden, mask_pos, labels, w_trans, b_trans, ln_gain, ln_bias, emb_table, b_vocab):
        n_rows, seq_len, width = hidden.shape
        n_masks = mask_pos.shape[1]
        shard_rows = emb_table.shape[0]
        n_own = n_rows * n_masks
        n_tokens = n_own * n_groups
        pad = -n_own % (SUBLANES * n_vp)
        me = lax.axis_index("dp")
        row_start = lax.axis_index("vp") * shard_rows
        vp = lax.axis_index("vp")

        slots = n_own + pad
        half = slots // n_vp
        label_row = jnp.pad(labels.reshape(1, n_own).astype(F32), ((0, 0), (0, width - n_own)), constant_values=-1.0)
        z, pre_act, u_own, sent = head(vp.reshape(1), mask_pos, hidden, w_trans, b_trans, ln_gain, ln_bias, label_row, slots, half)
        gathered = lax.all_gather(sent, ("vp", "dp"), axis=0, tiled=True)
        u_all = round_rows(gathered, slots)

        def token_order(rows):
            return jnp.swapaxes(rows.reshape(n_groups, n_vp, half), 0, 1).reshape(1, -1)

        own_slots = gathered.reshape(n_vp, n_groups, half, width)
        labels_all = token_order(own_slots[n_own // half, :, n_own % half, :slots].astype(jnp.int32) - row_start)

        logits, top, total = own_stats(u_own, emb_table, b_vocab)
        stats = jnp.pad(jnp.concatenate([top, total], axis=1).T, ((0, 0), (0, -slots % 1024))).reshape(-1, LANES)
        stats = lax.all_gather(stats, ("vp", "dp"), axis=0, tiled=True).reshape(n_vp, n_groups, 2, -1)
        top = jnp.max(stats[:, :, 0], axis=0)
        log_norm = top + jnp.log(jnp.sum(stats[:, :, 1] * jnp.exp(stats[:, :, 0] - top), axis=0))
        lse = jnp.where(jnp.arange(log_norm.shape[1]) < n_own, log_norm + math.log(n_tokens), -NEGATIVE)[:, :slots]
        lse_all = token_order(lse)
        lse_own = lax.dynamic_slice_in_dim(lse, me, 1).reshape(slots, 1)
        norm_own = lax.dynamic_slice_in_dim(log_norm, me, 1)[:, :slots].reshape(slots, 1)
        label_col = jnp.pad((labels - row_start).reshape(n_own, 1), ((0, pad), (0, 0)), constant_values=-(2**30))
        du_part = own_du(logits, emb_table, lse_own, label_col, 1.0 / n_tokens, n_own)

        tiles = pl.cdiv(shard_rows, TILE_V)
        k = GATHERED_TILES
        m = (tiles - n_groups * k) // 2
        core = lax.rem(me, 2)
        bias_col = b_vocab.reshape(shard_rows, 1)
        lse_all, du_part = lax.optimization_barrier((lse_all, du_part))
        part1, db1 = emb_grad((me * k).reshape(1), k, 0, 1.0 / n_tokens, labels_all, lse_all, emb_table, bias_col, u_all)
        mine = (n_groups * k + core * m).reshape(1)
        theirs = (n_groups * k + (1 - core) * m).reshape(1)
        rows1 = lax.all_gather(jnp.concatenate([part1, jnp.pad(jnp.pad(jnp.sum(db1, axis=1), (0, -k * TILE_V % width)).reshape(-1, width), ((0, 8 - pl.cdiv(k * TILE_V, width)), (0, 0)))]), "dp", axis=0)
        swap = [(i, i ^ 1) for i in range(n_groups)]
        du_other = lax.ppermute(du_part, "vp", [(0, 1), (1, 0)])
        sum_in, dz = head_grad(du_part, du_other, pre_act, z, w_trans, ln_gain, norm_own, n_own, n_tokens)
        lse_all, sum_in = lax.optimization_barrier((lse_all, sum_in))

        part2, full, db2 = emb_grad(mine, m, shard_rows, 1.0 / n_tokens, labels_all, lse_all, emb_table, bias_col, u_all)
        rows2 = lax.ppermute(part2, "dp", swap)
        db2 = jnp.sum(db2, axis=1)
        db2_other = lax.ppermute(db2, "dp", swap)
        rows1, sum_in = lax.optimization_barrier((rows1, sum_in))
        sums = lax.psum(sum_in, "dp")

        full = put_rows(jnp.zeros((1,), jnp.int32), rows1, full, n_groups, k)
        d_emb_table = put_rows(theirs, rows2[None], full, 1, m)
        db1_all = rows1[:, k * TILE_V :].reshape(n_groups, -1)[:, : k * TILE_V].reshape(-1)
        db_first, db_last = jnp.where(core == 0, db2, db2_other), jnp.where(core == 0, db2_other, db2)
        d_b_vocab = jnp.concatenate([db1_all, db_first, db_last])[:shard_rows]

        d_hidden = scatter(mask_pos, dz, seq_len)
        return sums[width + 3, 0], d_hidden, sums[:width], sums[width], sums[width + 1], sums[width + 2], d_emb_table, d_b_vocab

    in_specs = (P("dp", None, None), P("dp", None), P("dp", None), P(None, None), P(None), P(None), P(None), P("vp", None), P("vp"))
    out_specs = (P(), P("dp", None, None), P(None, None), P(None), P(None), P(None), P("vp", None), P("vp"))

    return jax.shard_map(local_step, mesh=mesh, in_specs=in_specs, out_specs=out_specs, check_vma=False)
```

```python
import functools
import math

import jax
import jax.numpy as jnp
from jax import lax
from jax.experimental import pallas as pl
from jax.experimental.pallas import tpu as pltpu
from jax.sharding import PartitionSpec as P


LN_EPS = 1e-5
F32 = jnp.float32
BF16 = jnp.bfloat16
NT = (((1,), (1,)), ((), ()))
LANES = 128
SUBLANES = 16
ROWS = 128
NEGATIVE = -1e30
OWN_V = 512
TILE_V = 768
TILE_T = 512
FINISH_TILES = 2
GATHERED_TILES = 1


def gelu_parts(a):
    cdf = 0.5 * (1.0 + lax.erf(a * math.sqrt(0.5)))
    return cdf, a * cdf


def normalised(g):
    centered = g - jnp.mean(g, axis=-1, keepdims=True)
    scale = lax.rsqrt(jnp.mean(centered * centered, axis=-1, keepdims=True) + LN_EPS)
    return centered * scale, scale


def row_loop(rows, step, body):
    def run(i, carry):
        body(pl.multiple_of(i * step, step), step)
        return carry

    lax.fori_loop(0, rows // step, run, 0)
    if rows % step:
        body(rows - rows % step, rows % step)


def window_start(n_masks, c):
    return pl.multiple_of(n_masks * c // SUBLANES * SUBLANES, SUBLANES)


def head_kernel(n_masks, window, label_at, vp_ref, key_ref, hidden_ref, w_ref, b_ref, gain_ref, beta_ref, label_ref,
                z_ref, pre_ref, u_ref, sent_ref, z_acc, u_acc):
    c = pl.program_id(0)
    slots, seq_len = z_ref.shape[0], hidden_ref.shape[0]
    half = sent_ref.shape[0]

    @pl.when(c == 0)
    def _():
        z_acc[...] = jnp.zeros_like(z_acc)

    here = pl.ds(window_start(n_masks, c), window)
    ids = c * seq_len + lax.broadcasted_iota(jnp.int32, (window, seq_len), 1)
    pick = (key_ref[here, :] == ids).astype(F32).astype(BF16)
    z_acc[here, :] += jnp.dot(pick, hidden_ref[...], preferred_element_type=F32)

    @pl.when(c == pl.num_programs(0) - 1)
    def _():
        z_ref[...] = z_acc[...].astype(BF16)
        pre_ref[...] = jnp.dot(z_ref[...], w_ref[...], preferred_element_type=F32) + b_ref[...]

        def norm(r, count):
            at = pl.ds(r, count)
            _, g = gelu_parts(pre_ref[at, :])
            xhat, _ = normalised(g)
            u = xhat * gain_ref[...] + beta_ref[...]
            u_acc[at, :] = u
            u_ref[at, :] = u.astype(BF16)

        row_loop(slots, ROWS, norm)
        sent_ref[...] = u_acc[pl.ds(pl.multiple_of(vp_ref[0] * half, SUBLANES), half), :]

        @pl.when(vp_ref[0] == label_at // half)
        def _():
            sent_ref[label_at % half : label_at % half + 1, :] = label_ref[...]


def head(vp, mask_pos, hidden, w, b, gain, beta, label_row, slots, half):
    n_rows, seq_len, width = hidden.shape
    n_masks = mask_pos.shape[1]
    key = (mask_pos + seq_len * jnp.arange(n_rows)[:, None]).reshape(-1, 1)
    key = jnp.pad(key, ((0, slots - n_rows * n_masks), (0, 0)), constant_values=-1)
    whole = lambda rows, cols: pl.BlockSpec((rows, cols), lambda c, v: (0, 0), pipeline_mode=pl.Buffered(1))
    out = lambda rows: pl.BlockSpec((rows, width), lambda c, v: (0, 0), pipeline_mode=pl.Buffered(1))
    return pl.pallas_call(
        functools.partial(head_kernel, n_masks, window_rows(n_masks), n_rows * n_masks),
        name="head",
        grid_spec=pltpu.PrefetchScalarGridSpec(
            num_scalar_prefetch=1,
            grid=(n_rows,),
            in_specs=[whole(slots, 1), pl.BlockSpec((None, seq_len, width), lambda c, v: (c, 0, 0)), whole(width, width)] + [whole(1, width)] * 4,
            out_specs=[out(slots), out(slots), out(slots), out(half)],
            scratch_shapes=[pltpu.VMEM((slots, width), F32), pltpu.VMEM((slots, width), F32)],
        ),
        out_shape=[
            jax.ShapeDtypeStruct((slots, width), BF16),
            jax.ShapeDtypeStruct((slots, width), F32),
            jax.ShapeDtypeStruct((slots, width), BF16),
            jax.ShapeDtypeStruct((half, width), F32),
        ],
        compiler_params=pltpu.CompilerParams(vmem_limit_bytes=50_000_000),
        cost_estimate=pl.CostEstimate(flops=2 * slots * width * width * 4, bytes_accessed=hidden.size * 2, transcendentals=slots * width),
    )(vp, key, hidden, w, b.reshape(1, width), gain.reshape(1, width), beta.reshape(1, width), label_row)


def row_blocks(rows, n):
    sixteenths = rows // SUBLANES
    sizes = [(sixteenths // n + (i < sixteenths % n)) * SUBLANES for i in range(n)]
    return [slice(sum(sizes[:i]), sum(sizes[: i + 1])) for i in range(n)]


def stats_kernel(emb_ref, bias_ref, u_ref, logit_ref, max_ref, sum_ref, m_acc, l_acc):
    i = pl.program_id(0)

    @pl.when(i == 0)
    def _():
        m_acc[...] = jnp.full_like(m_acc, NEGATIVE)
        l_acc[...] = jnp.zeros_like(l_acc)

    blocks = row_blocks(u_ref.shape[0], 2)

    def logits(rows):
        logit_ref[rows, :] = lax.dot_general(u_ref[rows, :], emb_ref[...], NT, preferred_element_type=F32) + bias_ref[...]

    def stats(rows):
        tiles = [logit_ref[rows, LANES * j : LANES * (j + 1)] for j in range(logit_ref.shape[1] // LANES)]
        old = m_acc[rows, :]
        top = functools.reduce(jnp.maximum, tiles, old)
        l_acc[rows, :] = l_acc[rows, :] * jnp.exp(old - top) + sum(jnp.exp(x - top) for x in tiles)
        m_acc[rows, :] = top

    logits(blocks[0])
    for before, rows in zip(blocks, blocks[1:]):
        logits(rows)
        stats(before)
    stats(blocks[-1])

    @pl.when(i == pl.num_programs(0) - 1)
    def _():
        top = jnp.max(m_acc[...], axis=-1, keepdims=True)
        max_ref[...] = top
        sum_ref[...] = jnp.sum(l_acc[...] * jnp.exp(m_acc[...] - top), axis=-1, keepdims=True)


def tile_of_rows(shard_rows, width):
    last = shard_rows - OWN_V
    return pl.BlockSpec((pl.Element(OWN_V), pl.Element(width)), lambda i: (pl.multiple_of(jnp.minimum(i * OWN_V, last), SUBLANES), 0))


def in_tiles(row, fill):
    n = row.shape[0]
    full = n // OWN_V
    again = OWN_V - n % OWN_V
    last = jnp.concatenate([jnp.full((again,), fill, row.dtype), row[full * OWN_V :]])
    return jnp.concatenate([row[: full * OWN_V], last]).reshape(full + 1, 1, OWN_V)


def own_stats(u, emb, bias):
    slots, width = u.shape
    bias = in_tiles(bias, NEGATIVE)
    n = bias.shape[0]
    col = pl.BlockSpec((slots, 1), lambda i: (0, 0))
    return pl.pallas_call(
        stats_kernel,
        name="own_stats",
        grid=(n,),
        in_specs=[
            tile_of_rows(emb.shape[0], width),
            pl.BlockSpec((None, 1, OWN_V), lambda i: (i, 0, 0)),
            pl.BlockSpec((slots, width), lambda i: (0, 0), pipeline_mode=pl.Buffered(1)),
        ],
        out_specs=[pl.BlockSpec((slots, OWN_V), lambda i: (0, i)), col, col],
        out_shape=[jax.ShapeDtypeStruct((slots, n * OWN_V), F32)] + [jax.ShapeDtypeStruct((slots, 1), F32)] * 2,
        scratch_shapes=[pltpu.VMEM((slots, LANES), F32)] * 2,
        compiler_params=pltpu.CompilerParams(vmem_limit_bytes=50_000_000),
        cost_estimate=pl.CostEstimate(flops=2 * slots * n * OWN_V * width, bytes_accessed=slots * n * OWN_V * 4, transcendentals=slots * n * OWN_V),
    )(emb, bias, u)


def du_kernel(inv_n, spare, logit_ref, emb_ref, ids_ref, lse_ref, lab_ref, du_ref, lse_b, lab_b, hit_acc, acc):
    i = pl.program_id(0)
    blocks = row_blocks(lse_ref.shape[0], 2)

    @pl.when(i == 0)
    def _():
        acc[...] = jnp.zeros_like(acc)
        hit_acc[...] = jnp.zeros_like(hit_acc)
        lse_b[...] = jnp.broadcast_to(lse_ref[...], lse_b.shape)
        lab_b[...] = jnp.broadcast_to(lab_ref[...], lab_b.shape)

    def grad(rows):
        parts = []
        hits = hit_acc[rows, :]
        for j in range(logit_ref.shape[1] // LANES):
            cols = slice(LANES * j, LANES * (j + 1))
            x = logit_ref[rows, cols]
            hit = ids_ref[:, cols] == lab_b[rows, :]
            hits = hits + jnp.where(hit, x, 0.0)
            parts.append((jnp.exp(x - lse_b[rows, :]) - jnp.where(hit, inv_n, 0.0)).astype(BF16))
        hit_acc[rows, :] = hits
        return jnp.concatenate(parts, axis=1)

    for rows in blocks:
        acc[rows, :] += jnp.dot(grad(rows), emb_ref[...], preferred_element_type=F32)

    @pl.when(i == pl.num_programs(0) - 1)
    def _():
        du_ref[...] = acc[...].astype(BF16).astype(F32)
        du_ref[spare : spare + 1, :LANES] = jnp.sum(hit_acc[...], axis=0, keepdims=True)


def own_du(logits, emb, lse, labels, inv_n, n_own):
    slots, width = lse.shape[0], emb.shape[1]
    ids = in_tiles(jnp.arange(emb.shape[0], dtype=jnp.int32), 2**30)
    n = ids.shape[0]
    col = pl.BlockSpec((slots, 1), lambda i: (0, 0), pipeline_mode=pl.Buffered(1))
    return pl.pallas_call(
        functools.partial(du_kernel, inv_n, n_own),
        name="own_du",
        grid=(n,),
        in_specs=[
            pl.BlockSpec((slots, OWN_V), lambda i: (0, i)),
            tile_of_rows(emb.shape[0], width),
            pl.BlockSpec((None, 1, OWN_V), lambda i: (i, 0, 0)),
            col,
            col,
        ],
        out_specs=pl.BlockSpec((slots, width), lambda i: (0, 0), pipeline_mode=pl.Buffered(1)),
        out_shape=jax.ShapeDtypeStruct((slots, width), F32),
        scratch_shapes=[pltpu.VMEM((slots, LANES), F32), pltpu.VMEM((slots, LANES), jnp.int32), pltpu.VMEM((slots, LANES), F32), pltpu.VMEM((slots, width), F32)],
        compiler_params=pltpu.CompilerParams(vmem_limit_bytes=50_000_000),
        cost_estimate=pl.CostEstimate(flops=2 * slots * n * OWN_V * width, bytes_accessed=slots * n * OWN_V * 4, transcendentals=slots * n * OWN_V),
    )(logits, emb, ids, lse, labels)


def head_grad_kernel(n_own, n_tokens, du0_ref, du1_ref, pre_ref, z_ref, w_ref, gain_ref, lse_ref, sums_ref, dz_ref, dab_ref, b_acc, g_acc, o_acc):
    slots, width = pre_ref.shape
    for a in (b_acc, g_acc, o_acc):
        a[...] = jnp.zeros_like(a)

    def fold(x):
        return functools.reduce(jnp.add, [x[8 * j : 8 * (j + 1), :] for j in range(x.shape[0] // 8)])

    def body(r, count):
        at = pl.ds(r, count)
        real = r + lax.broadcasted_iota(jnp.int32, (count, width), 0) < n_own
        du = jnp.where(real, du0_ref[at, :] + du1_ref[at, :], 0.0)
        a = pre_ref[at, :]
        cdf, g = gelu_parts(a)
        xhat, scale = normalised(g)
        dx = du * gain_ref[...]
        mean_dx = jnp.mean(dx, axis=-1, keepdims=True)
        mean_dxx = jnp.mean(dx * xhat, axis=-1, keepdims=True)
        dg = scale * (dx - mean_dx - xhat * mean_dxx)
        da = dg * (cdf + a * (math.sqrt(0.5 / math.pi) * jnp.exp(-0.5 * a * a)))
        b_acc[...] += fold(da)
        g_acc[...] += fold(du * xhat)
        o_acc[...] += fold(du)
        dab_ref[at, :] = da.astype(BF16)

    row_loop(slots, ROWS, body)
    sums_ref[:width, :] = lax.dot_general(z_ref[...], dab_ref[...], (((0,), (0,)), ((), ())), preferred_element_type=F32)
    dz_ref[...] = lax.dot_general(dab_ref[...], w_ref[...], NT, preferred_element_type=F32).astype(BF16)
    real = lax.broadcasted_iota(jnp.int32, (slots, 1), 0) < n_own
    norms = jnp.sum(jnp.where(real, lse_ref[...], 0.0))
    target = jnp.sum(du0_ref[n_own : n_own + 1, :LANES] + du1_ref[n_own : n_own + 1, :LANES])
    rows = lax.broadcasted_iota(jnp.int32, (8, width), 0)
    tail = jnp.where(rows == 3, (norms - target) / n_tokens, 0.0)
    for j, a in enumerate((b_acc, g_acc, o_acc)):
        tail = jnp.where(rows == j, jnp.sum(a[...], axis=0, keepdims=True), tail)
    sums_ref[width:, :] = tail


def head_grad(du0, du1, pre, z, w, gain, lse, n_own, n_tokens):
    slots, width = pre.shape
    vmem = pl.BlockSpec(memory_space=pltpu.VMEM)
    return pl.pallas_call(
        functools.partial(head_grad_kernel, n_own, n_tokens),
        name="head_grad",
        in_specs=[vmem] * 7,
        out_specs=[vmem] * 2,
        out_shape=[jax.ShapeDtypeStruct((width + 8, width), F32), jax.ShapeDtypeStruct((slots, width), BF16)],
        scratch_shapes=[pltpu.VMEM((slots, width), BF16)] + [pltpu.VMEM((8, width), F32)] * 3,
        compiler_params=pltpu.CompilerParams(vmem_limit_bytes=55_000_000),
        cost_estimate=pl.CostEstimate(flops=8 * slots * width * width, bytes_accessed=slots * width * 18, transcendentals=slots * width),
    )(du0, du1, pre, z, w, gain.reshape(1, width), lse)


def window_rows(n_masks):
    return -(-(n_masks + SUBLANES - 1) // SUBLANES) * SUBLANES


def scatter_kernel(n_masks, window, pos_ref, dz_ref, out_ref):
    c = pl.program_id(0)
    seq_len = out_ref.shape[0]
    hit = pos_ref[...] == lax.broadcasted_iota(jnp.int32, (seq_len, window), 0)
    rows = dz_ref[pl.ds(window_start(n_masks, c), window), :]
    out_ref[...] = jnp.dot(hit.astype(F32).astype(BF16), rows, preferred_element_type=F32).astype(BF16)


def scatter(mask_pos, dz, seq_len):
    n_rows, n_masks = mask_pos.shape
    width = dz.shape[1]
    window = window_rows(n_masks)
    lead = [n_masks * c % SUBLANES for c in range(n_rows)]
    pos = jnp.stack([jnp.pad(mask_pos[c], (a, window - n_masks - a), constant_values=-1) for c, a in enumerate(lead)])
    return pl.pallas_call(
        functools.partial(scatter_kernel, n_masks, window),
        name="scatter",
        grid=(n_rows,),
        in_specs=[pl.BlockSpec((None, 1, window), lambda c: (c, 0, 0)), pl.BlockSpec(dz.shape, lambda c: (0, 0), pipeline_mode=pl.Buffered(1))],
        out_specs=pl.BlockSpec((None, seq_len, width), lambda c: (c, 0, 0)),
        out_shape=jax.ShapeDtypeStruct((n_rows, seq_len, width), BF16),
        cost_estimate=pl.CostEstimate(flops=2 * n_rows * seq_len * window * width, bytes_accessed=n_rows * seq_len * width * 2, transcendentals=0),
    )(pos[:, None, :], dz)


def emb_grad_kernel(tc, n, tail, inv_n, bv, grid_tiles, mode, *refs):
    off_ref, lab_ref, lse_ref, emb_ref, bias_ref, u_hbm, *rest = refs
    if mode == "first":
        out_ref, u_out, u_ref, s0, s1, bb_ref, db_acc, in_sem, stage, out_sem = rest
    elif mode == "place":
        acc, db_ref, full_ref, u_ref, s0, s1, bb_ref, db_acc, in_sem = rest
    else:
        rows1, rows2, _, acc, db_ref, full_ref, u_ref, s0, s1, bb_ref, db_acc, in_sem, cbuf, cin_sem, cout_sem, put_sem = rest
    if mode == "first":
        acc, db_ref = out_ref.at[pl.ds(0, bv), :], out_ref.at[pl.ds(bv, 1), pl.ds(0, bv)]
    step = pl.program_id(0)
    tile = off_ref[0] + step
    row0 = tile * bv
    last = n + (1 if tail else 0)

    def at(i):
        return i * tc if isinstance(i, int) else pl.multiple_of(i * tc, tc)

    def size(i):
        return tail if isinstance(i, int) and i == n else tc

    def fetch(i):
        slot = stage.at[i % 4 if isinstance(i, int) else lax.rem(i, 4)] if mode == "first" else u_ref.at[pl.ds(at(i), size(i)), :]
        if mode == "first" and size(i) != tc:
            slot = slot.at[pl.ds(0, size(i)), :]
        return pltpu.make_async_copy(u_hbm.at[pl.ds(at(i), size(i)), :], slot, in_sem.at[i])

    def hand_on(i):
        here = pl.ds(at(i), size(i))
        return pltpu.make_async_copy(u_ref.at[here, :], u_out.at[here, :], out_sem.at[i])

    def arrive(i):
        fetch(i).wait()

    def rounded(i):
        slot = i % 4 if isinstance(i, int) else lax.rem(i, 4)
        u_ref[pl.ds(at(i), size(i)), :] = stage[slot, : size(i), :].astype(BF16)

    def dot1(i):
        return lax.dot_general(emb_ref[...], u_ref[pl.ds(at(i), size(i)), :], NT, preferred_element_type=F32)

    def grad(s_ref, i):
        ids = row0 + lax.broadcasted_iota(jnp.int32, (bv, LANES), 0)
        total = None
        parts = []
        for j in range(size(i) // LANES):
            cols = pl.ds(at(i) + LANES * j, LANES)
            x = s_ref[:, LANES * j : LANES * (j + 1)] + bb_ref[...] - lse_ref[:, cols]
            g = jnp.exp(x) - jnp.where(ids == lab_ref[:, cols], inv_n, 0.0)
            total = g if total is None else total + g
            parts.append(g.astype(BF16))
        db_acc[...] += total
        return jnp.concatenate(parts, axis=1)

    def dot2(s_ref, i):
        acc[...] += jnp.dot(grad(s_ref, i), u_ref[pl.ds(at(i), size(i)), :], preferred_element_type=F32)

    if mode == "first":
        for i in range(4):
            fetch(i).start()
    else:

        @pl.when(step == 0)
        def _():
            for i in range(last):
                fetch(i).start()

    bb_ref[...] = jnp.broadcast_to(bias_ref[...], (LANES, bv)).T
    db_acc[...] = jnp.zeros_like(db_acc)
    acc[...] = jnp.zeros_like(acc)

    def need(*chunks):
        if mode != "first":

            @pl.when(step == 0)
            def _():
                for i in chunks:
                    arrive(i)

    if mode == "first":
        for i in range(3):
            arrive(i)
            rounded(i)
            if i + 4 < last:
                fetch(i + 4).start()
    need(0)
    s0[...] = dot1(0)
    if mode == "first":
        hand_on(0).start()

    def two_chunks(a):
        if mode == "first":
            for i in (a + 3, a + 4):
                arrive(i)
            for i in (a + 1, a + 2):
                hand_on(i).start()
        elif mode == "finish":
            copy_blocks(step * (n // 2 - 1) + a // 2)
        need(a + 1, a + 2)
        s1[...] = dot1(a + 1)
        dot2(s0, a)
        if mode == "first":
            for i in (a + 3, a + 4):
                rounded(i)
        s0[...] = dot1(a + 2)
        dot2(s1, a + 1)
        if mode == "first":
            for i in (a + 7, a + 8):
                if isinstance(i, int):
                    if i < last:
                        fetch(i).start()
                else:
                    full_chunks = i < n
                    pl.when(full_chunks)(lambda i=i: fetch(i).start())
                    if tail:
                        pl.when(i == n)(lambda: fetch(n).start())

    def copy_blocks(t):
        n1, n2 = rows1.shape[0], rows2.shape[0] // bv
        t = jnp.int32(t)
        slot, other = lax.rem(t, 2), 1 - lax.rem(t, 2)
        put = lambda x, where: pltpu.make_async_copy(cbuf.at[x], full_ref.at[pl.ds(where, bv), :], cout_sem.at[x])
        take1 = lambda x, b: pltpu.make_async_copy(rows1.at[b, pl.ds(0, bv), :], cbuf.at[x], cin_sem.at[x])
        take2 = lambda x, b: pltpu.make_async_copy(rows2.at[pl.ds(pl.multiple_of(b * bv, bv), bv), :], cbuf.at[x], cin_sem.at[x])

        @pl.when((t >= 2) & (t < n1 + n2 + 2))
        def _():
            put(slot, 0).wait()

        @pl.when(t < n1)
        def _():
            take1(slot, t).start()

        @pl.when((t >= n1) & (t < n1 + n2))
        def _():
            take2(slot, t - n1).start()

        @pl.when((t >= 1) & (t < n1 + n2 + 1))
        def _():
            take1(other, 0).wait()
            where = jnp.where(t <= n1, t - 1, off_ref[1] + t - 1 - n1) * bv
            put(other, pl.multiple_of(where, bv)).start()

    def body(i, carry):
        two_chunks(2 * i)
        return carry

    trips = n // 2 - 1
    if mode == "first":
        lax.fori_loop(0, trips - 1, body, 0)
        two_chunks(2 * (trips - 1))
    else:
        lax.fori_loop(0, trips, body, 0)
    if mode == "first":
        for i in range(n - 1, last):
            hand_on(i).start()
    need(*range(n - 1, last))
    s1[...] = dot1(n - 1)
    dot2(s0, n - 2)
    if tail:
        s0[:, :tail] = dot1(n)
    dot2(s1, n - 1)
    if tail:
        dot2(s0, n)

    db_ref[...] = jnp.sum(db_acc[...].T, axis=0, keepdims=True)
    if mode == "first":
        for i in range(last):
            hand_on(i).wait()
    elif mode == "place":
        full_ref[...] = acc[...]
    else:
        rows = full_ref.shape[0]
        whole, part = rows // bv, rows % bv

        def put_tile(count):
            copy = pltpu.make_async_copy(acc.at[pl.ds(0, count), :], full_ref.at[pl.ds(pl.multiple_of(row0, bv), count), :], put_sem)
            copy.start()
            copy.wait()

        pl.when(tile < whole)(lambda: put_tile(bv))
        if part:
            pl.when(tile == whole)(lambda: put_tile(part))

        @pl.when(step == pl.num_programs(0) - 1)
        def _():
            for t in range(grid_tiles * trips, rows1.shape[0] + rows2.shape[0] // bv + 2):
                copy_blocks(t)


def emb_grad(mode, tiles, n_tiles, inv_n, labels, lse, emb, bias, u, *moved):
    n_tok, width = u.shape
    n, tail = divmod(n_tok, TILE_T)
    if n % 2:
        n, tail = n - 1, tail + TILE_T
    chunks = n + (1 if tail else 0)
    bv = TILE_V
    rows = n_tiles * bv
    once = pl.Buffered(1)
    anywhere = pl.BlockSpec(memory_space=pl.ANY)
    full = jax.ShapeDtypeStruct(emb.shape, F32)
    extra = 8 if mode == "first" else 0
    out_specs = [pl.BlockSpec((bv + extra, width), lambda i, o: (i, 0))]
    out_shape = [jax.ShapeDtypeStruct((n_tiles * (bv + extra), width), F32)]
    if mode != "first":
        out_specs.append(pl.BlockSpec((None, 1, bv), lambda i, o: (i, 0, 0)))
        out_shape.append(jax.ShapeDtypeStruct((n_tiles, 1, bv), F32))
    scratch = [
        pltpu.VMEM((n_tok, width), BF16),
        pltpu.VMEM((bv, TILE_T), F32),
        pltpu.VMEM((bv, TILE_T), F32),
        pltpu.VMEM((bv, LANES), F32),
        pltpu.VMEM((bv, LANES), F32),
        pltpu.SemaphoreType.DMA((chunks,)),
    ]
    if mode == "first":
        out_specs.append(anywhere)
        out_shape.append(jax.ShapeDtypeStruct(u.shape, BF16))
        scratch += [pltpu.VMEM((4, TILE_T, width), F32), pltpu.SemaphoreType.DMA((chunks,))]
    elif mode == "place":
        out_specs.append(pl.BlockSpec((bv, width), lambda i, o: (o[0] + i, 0)))
        out_shape.append(full)
    else:
        out_specs.append(anywhere)
        out_shape.append(full)
        scratch += [pltpu.VMEM((2, bv, width), F32), pltpu.SemaphoreType.DMA((2,)), pltpu.SemaphoreType.DMA((2,)), pltpu.SemaphoreType.DMA]
    grid_spec = pltpu.PrefetchScalarGridSpec(
        num_scalar_prefetch=1,
        grid=(n_tiles,),
        in_specs=[
            pl.BlockSpec((1, n_tok), lambda i, o: (0, 0), pipeline_mode=once),
            pl.BlockSpec((1, n_tok), lambda i, o: (0, 0), pipeline_mode=once),
            pl.BlockSpec((bv, width), lambda i, o: (o[0] + i, 0)),
            pl.BlockSpec((1, bv), lambda i, o: (0, o[0] + i)),
        ]
        + [anywhere] * (1 + len(moved)),
        out_specs=out_specs,
        scratch_shapes=scratch,
    )
    flops = 4 * rows * n_tok * width
    return pl.pallas_call(
        functools.partial(emb_grad_kernel, TILE_T, n, tail, inv_n, bv, n_tiles, mode),
        grid_spec=grid_spec,
        out_shape=out_shape,
        input_output_aliases={8: 2} if mode == "finish" else {},
        compiler_params=pltpu.CompilerParams(vmem_limit_bytes=62_000_000),
        cost_estimate=pl.CostEstimate(flops=flops, bytes_accessed=n_tok * width * 2 + rows * width * 6, transcendentals=rows * n_tok),
    )(tiles, labels, lse, emb, bias, u, *moved)


def copy_kernel(off_ref, src_ref, full_ref, out_ref):
    out_ref[...] = src_ref[...]


def put_rows(first_tile, src, full, n_src, n_tiles):
    bv, width = TILE_V, full.shape[1]
    return pl.pallas_call(
        copy_kernel,
        grid_spec=pltpu.PrefetchScalarGridSpec(
            num_scalar_prefetch=1,
            grid=(n_src, n_tiles),
            in_specs=[pl.BlockSpec((None, bv, width), lambda d, i, o: (d, i, 0)), pl.BlockSpec(memory_space=pl.ANY)],
            out_specs=pl.BlockSpec((bv, width), lambda d, i, o: (o[0] + d * n_tiles + i, 0)),
        ),
        out_shape=jax.ShapeDtypeStruct(full.shape, full.dtype),
        input_output_aliases={2: 0},
        cost_estimate=pl.CostEstimate(flops=n_src * n_tiles * bv * width, bytes_accessed=n_src * n_tiles * bv * width * 8, transcendentals=0),
    )(first_tile, src, full)


def solution(mesh):
    n_groups, n_vp = mesh.shape["dp"], mesh.shape["vp"]

    def local_step(hidden, mask_pos, labels, w_trans, b_trans, ln_gain, ln_bias, emb_table, b_vocab):
        n_rows, seq_len, width = hidden.shape
        n_masks = mask_pos.shape[1]
        shard_rows = emb_table.shape[0]
        n_own = n_rows * n_masks
        n_tokens = n_own * n_groups
        pad = -n_own % (SUBLANES * n_vp)
        me = lax.axis_index("dp")
        row_start = lax.axis_index("vp") * shard_rows
        vp = lax.axis_index("vp")

        slots = n_own + pad
        half = slots // n_vp
        label_row = jnp.pad(labels.reshape(1, n_own).astype(F32), ((0, 0), (0, width - n_own)), constant_values=-1.0)
        z, pre_act, u_own, sent = head(vp.reshape(1), mask_pos, hidden, w_trans, b_trans, ln_gain, ln_bias, label_row, slots, half)
        gathered = lax.all_gather(sent, ("vp", "dp"), axis=0, tiled=True)

        def token_order(rows):
            return jnp.swapaxes(rows.reshape(n_groups, n_vp, half), 0, 1).reshape(1, -1)

        own_slots = gathered.reshape(n_vp, n_groups, half, width)
        labels_all = token_order(own_slots[n_own // half, :, n_own % half, :slots].astype(jnp.int32) - row_start)

        logits, top, total = own_stats(u_own, emb_table, b_vocab)
        stats = jnp.pad(jnp.concatenate([top, total], axis=1).T, ((0, 0), (0, -slots % 1024))).reshape(-1, LANES)
        stats = lax.all_gather(stats, ("vp", "dp"), axis=0, tiled=True).reshape(n_vp, n_groups, 2, -1)
        top = jnp.max(stats[:, :, 0], axis=0)
        log_norm = top + jnp.log(jnp.sum(stats[:, :, 1] * jnp.exp(stats[:, :, 0] - top), axis=0))
        lse = jnp.where(jnp.arange(log_norm.shape[1]) < n_own, log_norm + math.log(n_tokens), -NEGATIVE)[:, :slots]
        lse_all = token_order(lse)
        lse_own = lax.dynamic_slice_in_dim(lse, me, 1).reshape(slots, 1)
        norm_own = lax.dynamic_slice_in_dim(log_norm, me, 1)[:, :slots].reshape(slots, 1)
        label_col = jnp.pad((labels - row_start).reshape(n_own, 1), ((0, pad), (0, 0)), constant_values=-(2**30))
        du_part = own_du(logits, emb_table, lse_own, label_col, 1.0 / n_tokens, n_own)

        tiles = pl.cdiv(shard_rows, TILE_V)
        k = GATHERED_TILES
        m = (tiles - n_groups * k) // 2
        core = lax.rem(me, 2)
        bias_row = b_vocab.reshape(1, shard_rows)
        lse_all, du_part = lax.optimization_barrier((lse_all, du_part))
        pair = lambda a, b: jnp.stack([a, b]).astype(jnp.int32)
        part1, u_all = emb_grad("first", pair(me * k, 0), k, 1.0 / n_tokens, labels_all, lse_all, emb_table, bias_row, gathered)
        du_other = lax.ppermute(du_part, "vp", [(0, 1), (1, 0)])
        rows1 = lax.all_gather(part1, "dp", axis=0)

        swap = [(i, i ^ 1) for i in range(n_groups)]
        mb = FINISH_TILES
        ma = m - mb
        mine = n_groups * k + core * m
        theirs = n_groups * k + (1 - core) * m
        part2a, db2a, full = emb_grad("place", pair(mine, theirs), ma, 1.0 / n_tokens, labels_all, lse_all, emb_table, bias_row, u_all)
        rows2a = lax.ppermute(part2a, "dp", swap)

        du_other, db2a = lax.optimization_barrier((du_other, db2a))
        sum_in, dz = head_grad(du_part, du_other, pre_act, z, w_trans, ln_gain, norm_own, n_own, n_tokens)
        sums = lax.psum(sum_in, "dp")

        lse_last, sum_in = lax.optimization_barrier((lse_all, sum_in))
        part2b, db2b, full = emb_grad("finish", pair(mine + ma, theirs), mb, 1.0 / n_tokens, labels_all, lse_last, emb_table, bias_row, u_all, rows1, rows2a, full)
        rows2b = lax.ppermute(part2b, "dp", swap)
        db2 = jnp.concatenate([db2a, db2b]).reshape(-1)
        db2_other = lax.ppermute(db2, "dp", swap)
        dz, db2 = lax.optimization_barrier((dz, db2))
        d_hidden = scatter(mask_pos, dz, seq_len)
        d_emb_table = put_rows((theirs + ma).reshape(1), rows2b[None], full, 1, mb)
        db1_all = rows1.reshape(n_groups * k, TILE_V + 8, width)[:, TILE_V, :TILE_V].reshape(-1)
        db_first, db_last = jnp.where(core == 0, db2, db2_other), jnp.where(core == 0, db2_other, db2)
        d_b_vocab = jnp.concatenate([db1_all, db_first, db_last])[:shard_rows]
        return sums[width + 3, 0], d_hidden, sums[:width], sums[width], sums[width + 1], sums[width + 2], d_emb_table, d_b_vocab

    in_specs = (P("dp", None, None), P("dp", None), P("dp", None), P(None, None), P(None), P(None), P(None), P("vp", None), P("vp"))
    out_specs = (P(), P("dp", None, None), P(None, None), P(None), P(None), P(None), P("vp", None), P("vp"))

    return jax.shard_map(local_step, mesh=mesh, in_specs=in_specs, out_specs=out_specs, check_vma=False)
```

```python
import functools
import math

import jax
import jax.numpy as jnp
from jax import lax
from jax.experimental import pallas as pl
from jax.experimental.pallas import tpu as pltpu
from jax.sharding import PartitionSpec as P


LN_EPS = 1e-5
F32 = jnp.float32
BF16 = jnp.bfloat16
NT = (((1,), (1,)), ((), ()))
LANES = 128
SUBLANES = 16
ROWS = 128
GROUP = 2
NEGATIVE = -1e30
OWN_V = 512
TILE_V = 768
TILE_T = 512
FINISH_TILES = 2
GATHERED_TILES = 1


def gelu_parts(a):
    cdf = 0.5 * (1.0 + lax.erf(a * math.sqrt(0.5)))
    return cdf, a * cdf


def normalised(g):
    centered = g - jnp.mean(g, axis=-1, keepdims=True)
    scale = lax.rsqrt(jnp.mean(centered * centered, axis=-1, keepdims=True) + LN_EPS)
    return centered * scale, scale


def row_loop(rows, step, body):
    def run(i, carry):
        body(pl.multiple_of(i * step, step), step)
        return carry

    lax.fori_loop(0, rows // step, run, 0)
    if rows % step:
        body(rows - rows % step, rows % step)


def window_start(n_masks, c):
    return pl.multiple_of(n_masks * c // SUBLANES * SUBLANES, SUBLANES)


def head_kernel(n_masks, window, label_at, vp_ref, key_ref, hidden_ref, w_ref, rows_ref,
                z_ref, pre_ref, u_ref, sent_ref, z_acc, u_acc):
    c = pl.program_id(0)
    slots, (group, seq_len, _) = z_ref.shape[0], hidden_ref.shape
    half = sent_ref.shape[0]

    @pl.when(c == 0)
    def _():
        z_acc[...] = jnp.zeros_like(z_acc)

    for q in range(group):
        row = c * group + q
        here = pl.ds(window_start(n_masks, row), window)
        ids = row * seq_len + lax.broadcasted_iota(jnp.int32, (window, seq_len), 1)
        pick = (key_ref[here, :] == ids).astype(F32).astype(BF16)
        z_acc[here, :] += jnp.dot(pick, hidden_ref[q], preferred_element_type=F32)

    @pl.when(c == pl.num_programs(0) - 1)
    def _():
        z_ref[...] = z_acc[...].astype(BF16)
        pre_ref[...] = jnp.dot(z_ref[...], w_ref[...], preferred_element_type=F32) + rows_ref[0:1, :]

        def norm(r, count):
            at = pl.ds(r, count)
            _, g = gelu_parts(pre_ref[at, :])
            xhat, _ = normalised(g)
            u = xhat * rows_ref[1:2, :] + rows_ref[2:3, :]
            u_acc[at, :] = u
            u_ref[at, :] = u.astype(BF16)

        row_loop(slots, ROWS, norm)
        sent_ref[...] = u_acc[pl.ds(pl.multiple_of(vp_ref[0] * half, SUBLANES), half), :]

        @pl.when(vp_ref[0] == label_at // half)
        def _():
            sent_ref[label_at % half : label_at % half + 1, :] = rows_ref[3:4, :]


def head(vp, mask_pos, hidden, w, b, gain, beta, label_row, slots, half):
    n_rows, seq_len, width = hidden.shape
    n_masks = mask_pos.shape[1]
    key = (mask_pos + seq_len * jnp.arange(n_rows)[:, None]).reshape(-1, 1)
    key = jnp.pad(key, ((0, slots - n_rows * n_masks), (0, 0)), constant_values=-1)
    whole = lambda rows, cols: pl.BlockSpec((rows, cols), lambda c, v: (0, 0), pipeline_mode=pl.Buffered(1))
    out = lambda rows: pl.BlockSpec((rows, width), lambda c, v: (0, 0), pipeline_mode=pl.Buffered(1))
    return pl.pallas_call(
        functools.partial(head_kernel, n_masks, window_rows(n_masks), n_rows * n_masks),
        name="head",
        grid_spec=pltpu.PrefetchScalarGridSpec(
            num_scalar_prefetch=1,
            grid=(n_rows // GROUP,),
            in_specs=[whole(slots, 1), pl.BlockSpec((GROUP, seq_len, width), lambda c, v: (c, 0, 0)), whole(width, width), whole(4, width)],
            out_specs=[out(slots), out(slots), out(slots), out(half)],
            scratch_shapes=[pltpu.VMEM((slots, width), F32), pltpu.VMEM((slots, width), F32)],
        ),
        out_shape=[
            jax.ShapeDtypeStruct((slots, width), BF16),
            jax.ShapeDtypeStruct((slots, width), F32),
            jax.ShapeDtypeStruct((slots, width), BF16),
            jax.ShapeDtypeStruct((half, width), F32),
        ],
        compiler_params=pltpu.CompilerParams(vmem_limit_bytes=50_000_000),
        cost_estimate=pl.CostEstimate(flops=2 * slots * width * width * 4, bytes_accessed=hidden.size * 2, transcendentals=slots * width),
    )(vp, key, hidden, w, jnp.concatenate([b[None], gain[None], beta[None], label_row]))


def row_blocks(rows, n):
    sixteenths = rows // SUBLANES
    sizes = [(sixteenths // n + (i < sixteenths % n)) * SUBLANES for i in range(n)]
    return [slice(sum(sizes[:i]), sum(sizes[: i + 1])) for i in range(n)]


def stats_kernel(emb_ref, bias_ref, u_ref, logit_ref, max_ref, sum_ref, m_acc, l_acc):
    i = pl.program_id(0)

    @pl.when(i == 0)
    def _():
        m_acc[...] = jnp.full_like(m_acc, NEGATIVE)
        l_acc[...] = jnp.zeros_like(l_acc)

    blocks = row_blocks(u_ref.shape[0], 2)

    def logits(rows):
        logit_ref[rows, :] = lax.dot_general(u_ref[rows, :], emb_ref[...], NT, preferred_element_type=F32) + bias_ref[...]

    def stats(rows):
        tiles = [logit_ref[rows, LANES * j : LANES * (j + 1)] for j in range(logit_ref.shape[1] // LANES)]
        old = m_acc[rows, :]
        top = functools.reduce(jnp.maximum, tiles, old)
        l_acc[rows, :] = l_acc[rows, :] * jnp.exp(old - top) + sum(jnp.exp(x - top) for x in tiles)
        m_acc[rows, :] = top

    logits(blocks[0])
    for before, rows in zip(blocks, blocks[1:]):
        logits(rows)
        stats(before)
    stats(blocks[-1])

    @pl.when(i == pl.num_programs(0) - 1)
    def _():
        top = jnp.max(m_acc[...], axis=-1, keepdims=True)
        max_ref[...] = top
        sum_ref[...] = jnp.sum(l_acc[...] * jnp.exp(m_acc[...] - top), axis=-1, keepdims=True)


def tile_of_rows(shard_rows, width):
    last = shard_rows - OWN_V
    return pl.BlockSpec((pl.Element(OWN_V), pl.Element(width)), lambda i: (pl.multiple_of(jnp.minimum(i * OWN_V, last), SUBLANES), 0))


def in_tiles(row, fill):
    n = row.shape[0]
    full = n // OWN_V
    again = OWN_V - n % OWN_V
    last = jnp.concatenate([jnp.full((again,), fill, row.dtype), row[full * OWN_V :]])
    return jnp.concatenate([row[: full * OWN_V], last]).reshape(full + 1, 1, OWN_V)


def own_stats(u, emb, bias):
    slots, width = u.shape
    bias = in_tiles(bias, NEGATIVE)
    n = bias.shape[0]
    col = pl.BlockSpec((slots, 1), lambda i: (0, 0))
    return pl.pallas_call(
        stats_kernel,
        name="own_stats",
        grid=(n,),
        in_specs=[
            tile_of_rows(emb.shape[0], width),
            pl.BlockSpec((None, 1, OWN_V), lambda i: (i, 0, 0)),
            pl.BlockSpec((slots, width), lambda i: (0, 0), pipeline_mode=pl.Buffered(1)),
        ],
        out_specs=[pl.BlockSpec((slots, OWN_V), lambda i: (0, i)), col, col],
        out_shape=[jax.ShapeDtypeStruct((slots, n * OWN_V), F32)] + [jax.ShapeDtypeStruct((slots, 1), F32)] * 2,
        scratch_shapes=[pltpu.VMEM((slots, LANES), F32)] * 2,
        compiler_params=pltpu.CompilerParams(vmem_limit_bytes=50_000_000),
        cost_estimate=pl.CostEstimate(flops=2 * slots * n * OWN_V * width, bytes_accessed=slots * n * OWN_V * 4, transcendentals=slots * n * OWN_V),
    )(emb, bias, u)


def du_kernel(inv_n, spare, logit_ref, emb_ref, ids_ref, lse_ref, lab_ref, du_ref, lse_b, lab_b, hit_acc, acc):
    i = pl.program_id(0)
    blocks = row_blocks(lse_ref.shape[0], 2)

    @pl.when(i == 0)
    def _():
        acc[...] = jnp.zeros_like(acc)
        hit_acc[...] = jnp.zeros_like(hit_acc)
        lse_b[...] = jnp.broadcast_to(lse_ref[...], lse_b.shape)
        lab_b[...] = jnp.broadcast_to(lab_ref[...], lab_b.shape)

    def grad(rows):
        parts = []
        hits = hit_acc[rows, :]
        for j in range(logit_ref.shape[1] // LANES):
            cols = slice(LANES * j, LANES * (j + 1))
            x = logit_ref[rows, cols]
            hit = ids_ref[:, cols] == lab_b[rows, :]
            hits = hits + jnp.where(hit, x, 0.0)
            parts.append((jnp.exp(x - lse_b[rows, :]) - jnp.where(hit, inv_n, 0.0)).astype(BF16))
        hit_acc[rows, :] = hits
        return jnp.concatenate(parts, axis=1)

    for rows in blocks:
        acc[rows, :] += jnp.dot(grad(rows), emb_ref[...], preferred_element_type=F32)

    @pl.when(i == pl.num_programs(0) - 1)
    def _():
        du_ref[...] = acc[...].astype(BF16).astype(F32)
        du_ref[spare : spare + 1, :LANES] = jnp.sum(hit_acc[...], axis=0, keepdims=True)


def own_du(logits, emb, lse, labels, inv_n, n_own):
    slots, width = lse.shape[0], emb.shape[1]
    ids = in_tiles(jnp.arange(emb.shape[0], dtype=jnp.int32), 2**30)
    n = ids.shape[0]
    col = pl.BlockSpec((slots, 1), lambda i: (0, 0), pipeline_mode=pl.Buffered(1))
    return pl.pallas_call(
        functools.partial(du_kernel, inv_n, n_own),
        name="own_du",
        grid=(n,),
        in_specs=[
            pl.BlockSpec((slots, OWN_V), lambda i: (0, i)),
            tile_of_rows(emb.shape[0], width),
            pl.BlockSpec((None, 1, OWN_V), lambda i: (i, 0, 0)),
            col,
            col,
        ],
        out_specs=pl.BlockSpec((slots, width), lambda i: (0, 0), pipeline_mode=pl.Buffered(1)),
        out_shape=jax.ShapeDtypeStruct((slots, width), F32),
        scratch_shapes=[pltpu.VMEM((slots, LANES), F32), pltpu.VMEM((slots, LANES), jnp.int32), pltpu.VMEM((slots, LANES), F32), pltpu.VMEM((slots, width), F32)],
        compiler_params=pltpu.CompilerParams(vmem_limit_bytes=50_000_000),
        cost_estimate=pl.CostEstimate(flops=2 * slots * n * OWN_V * width, bytes_accessed=slots * n * OWN_V * 4, transcendentals=slots * n * OWN_V),
    )(logits, emb, ids, lse, labels)


def head_grad_kernel(n_own, n_tokens, du0_ref, du1_ref, pre_ref, z_ref, w_ref, gain_ref, lse_ref, sums_ref, dz_ref, dab_ref, b_acc, g_acc, o_acc):
    slots, width = pre_ref.shape
    for a in (b_acc, g_acc, o_acc):
        a[...] = jnp.zeros_like(a)

    def fold(x):
        return functools.reduce(jnp.add, [x[8 * j : 8 * (j + 1), :] for j in range(x.shape[0] // 8)])

    def body(r, count):
        at = pl.ds(r, count)
        real = r + lax.broadcasted_iota(jnp.int32, (count, width), 0) < n_own
        du = jnp.where(real, du0_ref[at, :] + du1_ref[at, :], 0.0)
        a = pre_ref[at, :]
        cdf, g = gelu_parts(a)
        xhat, scale = normalised(g)
        dx = du * gain_ref[...]
        mean_dx = jnp.mean(dx, axis=-1, keepdims=True)
        mean_dxx = jnp.mean(dx * xhat, axis=-1, keepdims=True)
        dg = scale * (dx - mean_dx - xhat * mean_dxx)
        da = dg * (cdf + a * (math.sqrt(0.5 / math.pi) * jnp.exp(-0.5 * a * a)))
        b_acc[...] += fold(da)
        g_acc[...] += fold(du * xhat)
        o_acc[...] += fold(du)
        dab_ref[at, :] = da.astype(BF16)

    row_loop(slots, ROWS, body)
    sums_ref[:width, :] = lax.dot_general(z_ref[...], dab_ref[...], (((0,), (0,)), ((), ())), preferred_element_type=F32)
    dz_ref[...] = lax.dot_general(dab_ref[...], w_ref[...], NT, preferred_element_type=F32).astype(BF16)
    real = lax.broadcasted_iota(jnp.int32, (slots, 1), 0) < n_own
    norms = jnp.sum(jnp.where(real, lse_ref[...], 0.0))
    target = jnp.sum(du0_ref[n_own : n_own + 1, :LANES] + du1_ref[n_own : n_own + 1, :LANES])
    rows = lax.broadcasted_iota(jnp.int32, (8, width), 0)
    tail = jnp.where(rows == 3, (norms - target) / n_tokens, 0.0)
    for j, a in enumerate((b_acc, g_acc, o_acc)):
        tail = jnp.where(rows == j, jnp.sum(a[...], axis=0, keepdims=True), tail)
    sums_ref[width:, :] = tail


def head_grad(du0, du1, pre, z, w, gain, lse, n_own, n_tokens):
    slots, width = pre.shape
    vmem = pl.BlockSpec(memory_space=pltpu.VMEM)
    return pl.pallas_call(
        functools.partial(head_grad_kernel, n_own, n_tokens),
        name="head_grad",
        in_specs=[vmem] * 7,
        out_specs=[vmem] * 2,
        out_shape=[jax.ShapeDtypeStruct((width + 8, width), F32), jax.ShapeDtypeStruct((slots, width), BF16)],
        scratch_shapes=[pltpu.VMEM((slots, width), BF16)] + [pltpu.VMEM((8, width), F32)] * 3,
        compiler_params=pltpu.CompilerParams(vmem_limit_bytes=55_000_000),
        cost_estimate=pl.CostEstimate(flops=8 * slots * width * width, bytes_accessed=slots * width * 18, transcendentals=slots * width),
    )(du0, du1, pre, z, w, gain.reshape(1, width), lse)


def window_rows(n_masks):
    return -(-(n_masks + SUBLANES - 1) // SUBLANES) * SUBLANES


def scatter_kernel(n_masks, window, pos_ref, dz_ref, out_ref):
    group, seq_len, _ = out_ref.shape
    for q in range(group):
        row = pl.program_id(0) * group + q
        hit = pos_ref[q] == lax.broadcasted_iota(jnp.int32, (seq_len, window), 0)
        rows = dz_ref[pl.ds(window_start(n_masks, row), window), :]
        out_ref[q] = jnp.dot(hit.astype(F32).astype(BF16), rows, preferred_element_type=F32).astype(BF16)


def scatter(mask_pos, dz, seq_len):
    n_rows, n_masks = mask_pos.shape
    width = dz.shape[1]
    window = window_rows(n_masks)
    lead = [n_masks * c % SUBLANES for c in range(n_rows)]
    pos = jnp.stack([jnp.pad(mask_pos[c], (a, window - n_masks - a), constant_values=-1) for c, a in enumerate(lead)])
    return pl.pallas_call(
        functools.partial(scatter_kernel, n_masks, window),
        name="scatter",
        grid=(n_rows // GROUP,),
        in_specs=[pl.BlockSpec((GROUP, 1, window), lambda c: (c, 0, 0)), pl.BlockSpec(dz.shape, lambda c: (0, 0), pipeline_mode=pl.Buffered(1))],
        out_specs=pl.BlockSpec((GROUP, seq_len, width), lambda c: (c, 0, 0)),
        out_shape=jax.ShapeDtypeStruct((n_rows, seq_len, width), BF16),
        cost_estimate=pl.CostEstimate(flops=2 * n_rows * seq_len * window * width, bytes_accessed=n_rows * seq_len * width * 2, transcendentals=0),
    )(pos[:, None, :], dz)


def emb_grad_kernel(tc, n, tail, inv_n, bv, grid_tiles, mode, *refs):
    off_ref, lab_ref, lse_ref, emb_ref, bias_ref, u_hbm, *rest = refs
    if mode == "first":
        out_ref, u_out, u_ref, s0, s1, bb_ref, db_acc, in_sem, stage, out_sem = rest
    elif mode == "place":
        acc, db_ref, full_ref, u_ref, s0, s1, bb_ref, db_acc, in_sem = rest
    else:
        rows1, rows2, _, acc, db_ref, full_ref, u_ref, s0, s1, bb_ref, db_acc, in_sem, cbuf, cin_sem, cout_sem, put_sem = rest
    if mode == "first":
        acc, db_ref = out_ref.at[pl.ds(0, bv), :], out_ref.at[pl.ds(bv, 1), pl.ds(0, bv)]
    step = pl.program_id(0)
    tile = off_ref[0] + step
    row0 = tile * bv
    last = n + (1 if tail else 0)

    def at(i):
        return i * tc if isinstance(i, int) else pl.multiple_of(i * tc, tc)

    def size(i):
        return tail if isinstance(i, int) and i == n else tc

    def fetch(i):
        slot = stage.at[i % 4 if isinstance(i, int) else lax.rem(i, 4)] if mode == "first" else u_ref.at[pl.ds(at(i), size(i)), :]
        if mode == "first" and size(i) != tc:
            slot = slot.at[pl.ds(0, size(i)), :]
        return pltpu.make_async_copy(u_hbm.at[pl.ds(at(i), size(i)), :], slot, in_sem.at[i])

    def hand_on(i):
        here = pl.ds(at(i), size(i))
        return pltpu.make_async_copy(u_ref.at[here, :], u_out.at[here, :], out_sem.at[i])

    def arrive(i):
        fetch(i).wait()

    def rounded(i):
        slot = i % 4 if isinstance(i, int) else lax.rem(i, 4)
        u_ref[pl.ds(at(i), size(i)), :] = stage[slot, : size(i), :].astype(BF16)

    def dot1(i):
        return lax.dot_general(emb_ref[...], u_ref[pl.ds(at(i), size(i)), :], NT, preferred_element_type=F32)

    def grad(s_ref, i):
        ids = row0 + lax.broadcasted_iota(jnp.int32, (bv, LANES), 0)
        total = None
        parts = []
        for j in range(size(i) // LANES):
            cols = pl.ds(at(i) + LANES * j, LANES)
            x = s_ref[:, LANES * j : LANES * (j + 1)] + bb_ref[...] - lse_ref[:, cols]
            g = jnp.exp(x) - jnp.where(ids == lab_ref[:, cols], inv_n, 0.0)
            total = g if total is None else total + g
            parts.append(g.astype(BF16))
        db_acc[...] += total
        return jnp.concatenate(parts, axis=1)

    def dot2(s_ref, i):
        acc[...] += jnp.dot(grad(s_ref, i), u_ref[pl.ds(at(i), size(i)), :], preferred_element_type=F32)

    if mode == "first":
        for i in range(4):
            fetch(i).start()
    else:

        @pl.when(step == 0)
        def _():
            for i in range(last):
                fetch(i).start()

    bb_ref[...] = jnp.broadcast_to(bias_ref[...], (LANES, bv)).T
    db_acc[...] = jnp.zeros_like(db_acc)
    acc[...] = jnp.zeros_like(acc)

    def need(*chunks):
        if mode != "first":

            @pl.when(step == 0)
            def _():
                for i in chunks:
                    arrive(i)

    if mode == "first":
        for i in range(3):
            arrive(i)
            rounded(i)
            if i + 4 < last:
                fetch(i + 4).start()
    need(0)
    s0[...] = dot1(0)
    if mode == "first":
        hand_on(0).start()

    def two_chunks(a):
        if mode == "first":
            for i in (a + 3, a + 4):
                arrive(i)
            for i in (a + 1, a + 2):
                hand_on(i).start()
        elif mode == "finish":
            copy_blocks(step * (n // 2 - 1) + a // 2)
        need(a + 1, a + 2)
        s1[...] = dot1(a + 1)
        dot2(s0, a)
        if mode == "first":
            for i in (a + 3, a + 4):
                rounded(i)
        s0[...] = dot1(a + 2)
        dot2(s1, a + 1)
        if mode == "first":
            for i in (a + 7, a + 8):
                if isinstance(i, int):
                    if i < last:
                        fetch(i).start()
                else:
                    full_chunks = i < n
                    pl.when(full_chunks)(lambda i=i: fetch(i).start())
                    if tail:
                        pl.when(i == n)(lambda: fetch(n).start())

    def copy_blocks(t):
        n1, n2 = rows1.shape[0], rows2.shape[0] // bv
        t = jnp.int32(t)
        slot, other = lax.rem(t, 2), 1 - lax.rem(t, 2)
        put = lambda x, where: pltpu.make_async_copy(cbuf.at[x], full_ref.at[pl.ds(where, bv), :], cout_sem.at[x])
        take1 = lambda x, b: pltpu.make_async_copy(rows1.at[b, pl.ds(0, bv), :], cbuf.at[x], cin_sem.at[x])
        take2 = lambda x, b: pltpu.make_async_copy(rows2.at[pl.ds(pl.multiple_of(b * bv, bv), bv), :], cbuf.at[x], cin_sem.at[x])

        @pl.when((t >= 2) & (t < n1 + n2 + 2))
        def _():
            put(slot, 0).wait()

        @pl.when(t < n1)
        def _():
            take1(slot, t).start()

        @pl.when((t >= n1) & (t < n1 + n2))
        def _():
            take2(slot, t - n1).start()

        @pl.when((t >= 1) & (t < n1 + n2 + 1))
        def _():
            take1(other, 0).wait()
            where = jnp.where(t <= n1, t - 1, off_ref[1] + t - 1 - n1) * bv
            put(other, pl.multiple_of(where, bv)).start()

    def body(i, carry):
        two_chunks(2 * i)
        return carry

    trips = n // 2 - 1
    if mode == "first":
        lax.fori_loop(0, trips - 1, body, 0)
        two_chunks(2 * (trips - 1))
    else:
        lax.fori_loop(0, trips, body, 0)
    if mode == "first":
        for i in range(n - 1, last):
            hand_on(i).start()
    need(*range(n - 1, last))
    s1[...] = dot1(n - 1)
    dot2(s0, n - 2)
    if tail:
        s0[:, :tail] = dot1(n)
    dot2(s1, n - 1)
    if tail:
        dot2(s0, n)

    db_ref[...] = jnp.sum(db_acc[...].T, axis=0, keepdims=True)
    if mode == "first":
        for i in range(last):
            hand_on(i).wait()
    elif mode == "place":
        full_ref[...] = acc[...]
    else:
        rows = full_ref.shape[0]
        whole, part = rows // bv, rows % bv

        def put_tile(count):
            copy = pltpu.make_async_copy(acc.at[pl.ds(0, count), :], full_ref.at[pl.ds(pl.multiple_of(row0, bv), count), :], put_sem)
            copy.start()
            copy.wait()

        pl.when(tile < whole)(lambda: put_tile(bv))
        if part:
            pl.when(tile == whole)(lambda: put_tile(part))

        @pl.when(step == pl.num_programs(0) - 1)
        def _():
            for t in range(grid_tiles * trips, rows1.shape[0] + rows2.shape[0] // bv + 2):
                copy_blocks(t)


def emb_grad(mode, tiles, n_tiles, inv_n, labels, lse, emb, bias, u, *moved):
    n_tok, width = u.shape
    n, tail = divmod(n_tok, TILE_T)
    if n % 2:
        n, tail = n - 1, tail + TILE_T
    chunks = n + (1 if tail else 0)
    bv = TILE_V
    rows = n_tiles * bv
    once = pl.Buffered(1)
    anywhere = pl.BlockSpec(memory_space=pl.ANY)
    full = jax.ShapeDtypeStruct(emb.shape, F32)
    extra = 8 if mode == "first" else 0
    out_specs = [pl.BlockSpec((bv + extra, width), lambda i, o: (i, 0))]
    out_shape = [jax.ShapeDtypeStruct((n_tiles * (bv + extra), width), F32)]
    if mode != "first":
        out_specs.append(pl.BlockSpec((None, 1, bv), lambda i, o: (i, 0, 0)))
        out_shape.append(jax.ShapeDtypeStruct((n_tiles, 1, bv), F32))
    scratch = [
        pltpu.VMEM((n_tok, width), BF16),
        pltpu.VMEM((bv, TILE_T), F32),
        pltpu.VMEM((bv, TILE_T), F32),
        pltpu.VMEM((bv, LANES), F32),
        pltpu.VMEM((bv, LANES), F32),
        pltpu.SemaphoreType.DMA((chunks,)),
    ]
    if mode == "first":
        out_specs.append(anywhere)
        out_shape.append(jax.ShapeDtypeStruct(u.shape, BF16))
        scratch += [pltpu.VMEM((4, TILE_T, width), F32), pltpu.SemaphoreType.DMA((chunks,))]
    elif mode == "place":
        out_specs.append(pl.BlockSpec((bv, width), lambda i, o: (o[0] + i, 0)))
        out_shape.append(full)
    else:
        out_specs.append(anywhere)
        out_shape.append(full)
        scratch += [pltpu.VMEM((2, bv, width), F32), pltpu.SemaphoreType.DMA((2,)), pltpu.SemaphoreType.DMA((2,)), pltpu.SemaphoreType.DMA]
    grid_spec = pltpu.PrefetchScalarGridSpec(
        num_scalar_prefetch=1,
        grid=(n_tiles,),
        in_specs=[
            pl.BlockSpec((1, n_tok), lambda i, o: (0, 0), pipeline_mode=once),
            pl.BlockSpec((1, n_tok), lambda i, o: (0, 0), pipeline_mode=once),
            pl.BlockSpec((bv, width), lambda i, o: (o[0] + i, 0)),
            pl.BlockSpec((1, bv), lambda i, o: (0, o[0] + i)),
        ]
        + [anywhere] * (1 + len(moved)),
        out_specs=out_specs,
        scratch_shapes=scratch,
    )
    flops = 4 * rows * n_tok * width
    return pl.pallas_call(
        functools.partial(emb_grad_kernel, TILE_T, n, tail, inv_n, bv, n_tiles, mode),
        grid_spec=grid_spec,
        out_shape=out_shape,
        input_output_aliases={8: 2} if mode == "finish" else {},
        compiler_params=pltpu.CompilerParams(vmem_limit_bytes=62_000_000),
        cost_estimate=pl.CostEstimate(flops=flops, bytes_accessed=n_tok * width * 2 + rows * width * 6, transcendentals=rows * n_tok),
    )(tiles, labels, lse, emb, bias, u, *moved)


def copy_kernel(off_ref, src_ref, full_ref, out_ref):
    out_ref[...] = src_ref[...]


def put_rows(first_tile, src, full, n_src, n_tiles):
    bv, width = TILE_V, full.shape[1]
    return pl.pallas_call(
        copy_kernel,
        grid_spec=pltpu.PrefetchScalarGridSpec(
            num_scalar_prefetch=1,
            grid=(n_src, n_tiles),
            in_specs=[pl.BlockSpec((None, bv, width), lambda d, i, o: (d, i, 0)), pl.BlockSpec(memory_space=pl.ANY)],
            out_specs=pl.BlockSpec((bv, width), lambda d, i, o: (o[0] + d * n_tiles + i, 0)),
        ),
        out_shape=jax.ShapeDtypeStruct(full.shape, full.dtype),
        input_output_aliases={2: 0},
        cost_estimate=pl.CostEstimate(flops=n_src * n_tiles * bv * width, bytes_accessed=n_src * n_tiles * bv * width * 8, transcendentals=0),
    )(first_tile, src, full)


def solution(mesh):
    n_groups, n_vp = mesh.shape["dp"], mesh.shape["vp"]

    def local_step(hidden, mask_pos, labels, w_trans, b_trans, ln_gain, ln_bias, emb_table, b_vocab):
        n_rows, seq_len, width = hidden.shape
        n_masks = mask_pos.shape[1]
        shard_rows = emb_table.shape[0]
        n_own = n_rows * n_masks
        n_tokens = n_own * n_groups
        pad = -n_own % (SUBLANES * n_vp)
        me = lax.axis_index("dp")
        row_start = lax.axis_index("vp") * shard_rows
        vp = lax.axis_index("vp")

        slots = n_own + pad
        half = slots // n_vp
        label_row = jnp.pad(labels.reshape(1, n_own).astype(F32), ((0, 0), (0, width - n_own)), constant_values=-1.0)
        z, pre_act, u_own, sent = head(vp.reshape(1), mask_pos, hidden, w_trans, b_trans, ln_gain, ln_bias, label_row, slots, half)
        gathered = lax.all_gather(sent, ("vp", "dp"), axis=0, tiled=True)

        def token_order(rows):
            return jnp.swapaxes(rows.reshape(n_groups, n_vp, half), 0, 1).reshape(1, -1)

        own_slots = gathered.reshape(n_vp, n_groups, half, width)
        labels_all = token_order(own_slots[n_own // half, :, n_own % half, :slots].astype(jnp.int32) - row_start)

        logits, top, total = own_stats(u_own, emb_table, b_vocab)
        stats = jnp.pad(jnp.concatenate([top, total], axis=1).T, ((0, 0), (0, -slots % 1024))).reshape(-1, LANES)
        stats = lax.all_gather(stats, ("vp", "dp"), axis=0, tiled=True).reshape(n_vp, n_groups, 2, -1)
        top = jnp.max(stats[:, :, 0], axis=0)
        log_norm = top + jnp.log(jnp.sum(stats[:, :, 1] * jnp.exp(stats[:, :, 0] - top), axis=0))
        lse = jnp.where(jnp.arange(log_norm.shape[1]) < n_own, log_norm + math.log(n_tokens), -NEGATIVE)[:, :slots]
        lse_all = token_order(lse)
        lse_own = lax.dynamic_slice_in_dim(lse, me, 1).reshape(slots, 1)
        norm_own = lax.dynamic_slice_in_dim(log_norm, me, 1)[:, :slots].reshape(slots, 1)
        label_col = jnp.pad((labels - row_start).reshape(n_own, 1), ((0, pad), (0, 0)), constant_values=-(2**30))
        du_part = own_du(logits, emb_table, lse_own, label_col, 1.0 / n_tokens, n_own)

        tiles = pl.cdiv(shard_rows, TILE_V)
        k = GATHERED_TILES
        m = (tiles - n_groups * k) // 2
        core = lax.rem(me, 2)
        bias_row = b_vocab.reshape(1, shard_rows)
        lse_all, du_part = lax.optimization_barrier((lse_all, du_part))
        pair = lambda a, b: jnp.stack([a, b]).astype(jnp.int32)
        part1, u_all = emb_grad("first", pair(me * k, 0), k, 1.0 / n_tokens, labels_all, lse_all, emb_table, bias_row, gathered)
        du_other = lax.ppermute(du_part, "vp", [(0, 1), (1, 0)])
        rows1 = lax.all_gather(part1, "dp", axis=0)

        swap = [(i, i ^ 1) for i in range(n_groups)]
        mb = FINISH_TILES
        ma = m - mb
        mine = n_groups * k + core * m
        theirs = n_groups * k + (1 - core) * m
        part2a, db2a, full = emb_grad("place", pair(mine, theirs), ma, 1.0 / n_tokens, labels_all, lse_all, emb_table, bias_row, u_all)
        rows2a = lax.ppermute(part2a, "dp", swap)

        du_other, db2a = lax.optimization_barrier((du_other, db2a))
        sum_in, dz = head_grad(du_part, du_other, pre_act, z, w_trans, ln_gain, norm_own, n_own, n_tokens)
        sums = lax.psum(sum_in, "dp")

        d_hidden = scatter(mask_pos, dz, seq_len)
        lse_last, d_hidden = lax.optimization_barrier((lse_all, d_hidden))
        part2b, db2b, full = emb_grad("finish", pair(mine + ma, theirs), mb, 1.0 / n_tokens, labels_all, lse_last, emb_table, bias_row, u_all, rows1, rows2a, full)
        rows2b = lax.ppermute(part2b, "dp", swap)
        db2 = jnp.concatenate([db2a, db2b]).reshape(-1)
        db2_other = lax.ppermute(db2, "dp", swap)
        d_emb_table = put_rows((theirs + ma).reshape(1), rows2b[None], full, 1, mb)
        db1_all = rows1.reshape(n_groups * k, TILE_V + 8, width)[:, TILE_V, :TILE_V].reshape(-1)
        db_first, db_last = jnp.where(core == 0, db2, db2_other), jnp.where(core == 0, db2_other, db2)
        d_b_vocab = jnp.concatenate([db1_all, db_first, db_last])[:shard_rows]
        return sums[width + 3, 0], d_hidden, sums[:width], sums[width], sums[width + 1], sums[width + 2], d_emb_table, d_b_vocab

    in_specs = (P("dp", None, None), P("dp", None), P("dp", None), P(None, None), P(None), P(None), P(None), P("vp", None), P("vp"))
    out_specs = (P(), P("dp", None, None), P(None, None), P(None), P(None), P(None), P("vp", None), P("vp"))

    return jax.shard_map(local_step, mesh=mesh, in_specs=in_specs, out_specs=out_specs, check_vma=False)
```

```python
import functools
import math

import jax
import jax.numpy as jnp
from jax import lax
from jax.experimental import pallas as pl
from jax.experimental.pallas import tpu as pltpu
from jax.sharding import PartitionSpec as P


LN_EPS = 1e-5
F32 = jnp.float32
BF16 = jnp.bfloat16
NT = (((1,), (1,)), ((), ()))
LANES = 128
SUBLANES = 16
ROWS = 256
GROUP = 2
NEGATIVE = -1e30
OWN_V = 512
TILE_V = 768
TILE_T = 512
FINISH_TILES = 2
GATHERED_TILES = 1


def gelu_parts(a):
    cdf = 0.5 * (1.0 + lax.erf(a * math.sqrt(0.5)))
    return cdf, a * cdf


def normalised(g):
    centered = g - jnp.mean(g, axis=-1, keepdims=True)
    scale = lax.rsqrt(jnp.mean(centered * centered, axis=-1, keepdims=True) + LN_EPS)
    return centered * scale, scale


def row_loop(rows, step, body):
    def run(i, carry):
        body(pl.multiple_of(i * step, step), step)
        return carry

    lax.fori_loop(0, rows // step, run, 0)
    if rows % step:
        body(rows - rows % step, rows % step)


def window_start(n_masks, c):
    return pl.multiple_of(n_masks * c // SUBLANES * SUBLANES, SUBLANES)


def head_kernel(n_masks, window, vp_ref, key_ref, hidden_ref, w_ref, rows_ref,
                z_ref, pre_ref, u_ref, sent_ref, z_acc, u_acc):
    c = pl.program_id(0)
    slots, (group, seq_len, _) = z_ref.shape[0], hidden_ref.shape
    half = sent_ref.shape[0]

    @pl.when(c == 0)
    def _():
        z_acc[...] = jnp.zeros_like(z_acc)

    for q in range(group):
        row = c * group + q
        here = pl.ds(window_start(n_masks, row), window)
        ids = row * seq_len + lax.broadcasted_iota(jnp.int32, (window, seq_len), 1)
        pick = (key_ref[here, :] == ids).astype(F32).astype(BF16)
        z_acc[here, :] += jnp.dot(pick, hidden_ref[q], preferred_element_type=F32)

    @pl.when(c == pl.num_programs(0) - 1)
    def _():
        z_ref[...] = z_acc[...].astype(BF16)
        pre_ref[...] = jnp.dot(z_ref[...], w_ref[...], preferred_element_type=F32) + rows_ref[0:1, :]

        def norm(r, count):
            at = pl.ds(r, count)
            _, g = gelu_parts(pre_ref[at, :])
            xhat, _ = normalised(g)
            u = xhat * rows_ref[1:2, :] + rows_ref[2:3, :]
            u_acc[at, :] = u
            u_ref[at, :] = u.astype(BF16)

        row_loop(slots, ROWS, norm)
        sent_ref[...] = u_acc[pl.ds(pl.multiple_of(vp_ref[0] * half, SUBLANES), half), :]


def head(vp, mask_pos, hidden, w, b, gain, beta, slots, half):
    n_rows, seq_len, width = hidden.shape
    n_masks = mask_pos.shape[1]
    key = (mask_pos + seq_len * jnp.arange(n_rows)[:, None]).reshape(-1, 1)
    key = jnp.pad(key, ((0, slots - n_rows * n_masks), (0, 0)), constant_values=-1)
    whole = lambda rows, cols: pl.BlockSpec((rows, cols), lambda c, v: (0, 0), pipeline_mode=pl.Buffered(1))
    out = lambda rows: pl.BlockSpec((rows, width), lambda c, v: (0, 0), pipeline_mode=pl.Buffered(1))
    return pl.pallas_call(
        functools.partial(head_kernel, n_masks, window_rows(n_masks)),
        name="head",
        grid_spec=pltpu.PrefetchScalarGridSpec(
            num_scalar_prefetch=1,
            grid=(n_rows // GROUP,),
            in_specs=[whole(slots, 1), pl.BlockSpec((GROUP, seq_len, width), lambda c, v: (c, 0, 0)), whole(width, width), whole(3, width)],
            out_specs=[out(slots), out(slots), out(slots), out(half)],
            scratch_shapes=[pltpu.VMEM((slots, width), F32), pltpu.VMEM((slots, width), F32)],
        ),
        out_shape=[
            jax.ShapeDtypeStruct((slots, width), BF16),
            jax.ShapeDtypeStruct((slots, width), F32),
            jax.ShapeDtypeStruct((slots, width), BF16),
            jax.ShapeDtypeStruct((half, width), F32),
        ],
        compiler_params=pltpu.CompilerParams(vmem_limit_bytes=50_000_000),
        cost_estimate=pl.CostEstimate(flops=2 * slots * width * width * 4, bytes_accessed=hidden.size * 2, transcendentals=slots * width),
    )(vp, key, hidden, w, jnp.concatenate([b[None], gain[None], beta[None]]))


def row_blocks(rows, n):
    sixteenths = rows // SUBLANES
    sizes = [(sixteenths // n + (i < sixteenths % n)) * SUBLANES for i in range(n)]
    return [slice(sum(sizes[:i]), sum(sizes[: i + 1])) for i in range(n)]


def stats_kernel(emb_ref, bias_ref, u_ref, logit_ref, max_ref, sum_ref, m_acc, l_acc):
    i = pl.program_id(0)

    @pl.when(i == 0)
    def _():
        m_acc[...] = jnp.full_like(m_acc, NEGATIVE)
        l_acc[...] = jnp.zeros_like(l_acc)

    blocks = row_blocks(u_ref.shape[0], 2)

    def logits(rows):
        logit_ref[rows, :] = lax.dot_general(u_ref[rows, :], emb_ref[...], NT, preferred_element_type=F32) + bias_ref[...]

    def stats(rows):
        tiles = [logit_ref[rows, LANES * j : LANES * (j + 1)] for j in range(logit_ref.shape[1] // LANES)]
        old = m_acc[rows, :]
        top = functools.reduce(jnp.maximum, tiles, old)
        l_acc[rows, :] = l_acc[rows, :] * jnp.exp(old - top) + sum(jnp.exp(x - top) for x in tiles)
        m_acc[rows, :] = top

    logits(blocks[0])
    for before, rows in zip(blocks, blocks[1:]):
        logits(rows)
        stats(before)
    stats(blocks[-1])

    @pl.when(i == pl.num_programs(0) - 1)
    def _():
        top = jnp.max(m_acc[...], axis=-1, keepdims=True)
        max_ref[...] = top
        sum_ref[...] = jnp.sum(l_acc[...] * jnp.exp(m_acc[...] - top), axis=-1, keepdims=True)


def tile_of_rows(shard_rows, width):
    last = shard_rows - OWN_V
    return pl.BlockSpec((pl.Element(OWN_V), pl.Element(width)), lambda i: (pl.multiple_of(jnp.minimum(i * OWN_V, last), SUBLANES), 0))


def in_tiles(row, fill):
    n = row.shape[0]
    full = n // OWN_V
    again = OWN_V - n % OWN_V
    last = jnp.concatenate([jnp.full((again,), fill, row.dtype), row[full * OWN_V :]])
    return jnp.concatenate([row[: full * OWN_V], last]).reshape(full + 1, 1, OWN_V)


def own_stats(u, emb, bias):
    slots, width = u.shape
    bias = in_tiles(bias, NEGATIVE)
    n = bias.shape[0]
    col = pl.BlockSpec((slots, 1), lambda i: (0, 0))
    return pl.pallas_call(
        stats_kernel,
        name="own_stats",
        grid=(n,),
        in_specs=[
            tile_of_rows(emb.shape[0], width),
            pl.BlockSpec((None, 1, OWN_V), lambda i: (i, 0, 0)),
            pl.BlockSpec((slots, width), lambda i: (0, 0), pipeline_mode=pl.Buffered(1)),
        ],
        out_specs=[pl.BlockSpec((slots, OWN_V), lambda i: (0, i)), col, col],
        out_shape=[jax.ShapeDtypeStruct((slots, n * OWN_V), F32)] + [jax.ShapeDtypeStruct((slots, 1), F32)] * 2,
        scratch_shapes=[pltpu.VMEM((slots, LANES), F32)] * 2,
        compiler_params=pltpu.CompilerParams(vmem_limit_bytes=50_000_000),
        cost_estimate=pl.CostEstimate(flops=2 * slots * n * OWN_V * width, bytes_accessed=slots * n * OWN_V * 4, transcendentals=slots * n * OWN_V),
    )(emb, bias, u)


def du_kernel(inv_n, spare, logit_ref, emb_ref, ids_ref, lse_ref, lab_ref, du_ref, lse_b, lab_b, hit_acc, acc):
    i = pl.program_id(0)
    blocks = row_blocks(lse_ref.shape[0], 2)

    @pl.when(i == 0)
    def _():
        acc[...] = jnp.zeros_like(acc)
        hit_acc[...] = jnp.zeros_like(hit_acc)
        lse_b[...] = jnp.broadcast_to(lse_ref[...], lse_b.shape)
        lab_b[...] = jnp.broadcast_to(lab_ref[...], lab_b.shape)

    def grad(rows):
        parts = []
        hits = hit_acc[rows, :]
        for j in range(logit_ref.shape[1] // LANES):
            cols = slice(LANES * j, LANES * (j + 1))
            x = logit_ref[rows, cols]
            hit = ids_ref[:, cols] == lab_b[rows, :]
            hits = hits + jnp.where(hit, x, 0.0)
            parts.append((jnp.exp(x - lse_b[rows, :]) - jnp.where(hit, inv_n, 0.0)).astype(BF16))
        hit_acc[rows, :] = hits
        return jnp.concatenate(parts, axis=1)

    for rows in blocks:
        acc[rows, :] += jnp.dot(grad(rows), emb_ref[...], preferred_element_type=F32)

    @pl.when(i == pl.num_programs(0) - 1)
    def _():
        du_ref[...] = acc[...].astype(BF16).astype(F32)
        du_ref[spare : spare + 1, :LANES] = jnp.sum(hit_acc[...], axis=0, keepdims=True)


def own_du(logits, emb, lse, labels, inv_n, n_own):
    slots, width = lse.shape[0], emb.shape[1]
    ids = in_tiles(jnp.arange(emb.shape[0], dtype=jnp.int32), 2**30)
    n = ids.shape[0]
    col = pl.BlockSpec((slots, 1), lambda i: (0, 0), pipeline_mode=pl.Buffered(1))
    return pl.pallas_call(
        functools.partial(du_kernel, inv_n, n_own),
        name="own_du",
        grid=(n,),
        in_specs=[
            pl.BlockSpec((slots, OWN_V), lambda i: (0, i)),
            tile_of_rows(emb.shape[0], width),
            pl.BlockSpec((None, 1, OWN_V), lambda i: (i, 0, 0)),
            col,
            col,
        ],
        out_specs=pl.BlockSpec((slots, width), lambda i: (0, 0), pipeline_mode=pl.Buffered(1)),
        out_shape=jax.ShapeDtypeStruct((slots, width), F32),
        scratch_shapes=[pltpu.VMEM((slots, LANES), F32), pltpu.VMEM((slots, LANES), jnp.int32), pltpu.VMEM((slots, LANES), F32), pltpu.VMEM((slots, width), F32)],
        compiler_params=pltpu.CompilerParams(vmem_limit_bytes=50_000_000),
        cost_estimate=pl.CostEstimate(flops=2 * slots * n * OWN_V * width, bytes_accessed=slots * n * OWN_V * 4, transcendentals=slots * n * OWN_V),
    )(logits, emb, ids, lse, labels)


def head_grad_kernel(n_own, n_tokens, du0_ref, du1_ref, pre_ref, z_ref, w_ref, gain_ref, lse_ref, sums_ref, dz_ref, dab_ref, b_acc, g_acc, o_acc):
    step = pl.program_id(0)
    block, width = pre_ref.shape

    @pl.when(step == 0)
    def _():
        for a in (b_acc, g_acc, o_acc, sums_ref):
            a[...] = jnp.zeros_like(a)

    def fold(x):
        return functools.reduce(jnp.add, [x[8 * j : 8 * (j + 1), :] for j in range(x.shape[0] // 8)])

    def body(r, count):
        at = pl.ds(r, count)
        real = step * block + r + lax.broadcasted_iota(jnp.int32, (count, width), 0) < n_own
        du = jnp.where(real, du0_ref[at, :] + du1_ref[at, :], 0.0)
        a = pre_ref[at, :]
        cdf, g = gelu_parts(a)
        xhat, scale = normalised(g)
        dx = du * gain_ref[...]
        mean_dx = jnp.mean(dx, axis=-1, keepdims=True)
        mean_dxx = jnp.mean(dx * xhat, axis=-1, keepdims=True)
        dg = scale * (dx - mean_dx - xhat * mean_dxx)
        da = dg * (cdf + a * (math.sqrt(0.5 / math.pi) * jnp.exp(-0.5 * a * a)))
        b_acc[...] += fold(da)
        g_acc[...] += fold(du * xhat)
        o_acc[...] += fold(du)
        dab_ref[at, :] = da.astype(BF16)

    row_loop(block, ROWS, body)
    sums_ref[:width, :] += lax.dot_general(z_ref[...], dab_ref[...], (((0,), (0,)), ((), ())), preferred_element_type=F32)
    dz_ref[...] = lax.dot_general(dab_ref[...], w_ref[...], NT, preferred_element_type=F32).astype(BF16)

    @pl.when(step == pl.num_programs(0) - 1)
    def _():
        real = lax.broadcasted_iota(jnp.int32, lse_ref.shape, 0) < n_own
        norms = jnp.sum(jnp.where(real, lse_ref[...] - math.log(n_tokens), 0.0))
        spare = n_own % block
        target = jnp.sum(du0_ref[spare : spare + 1, :LANES] + du1_ref[spare : spare + 1, :LANES])
        rows = lax.broadcasted_iota(jnp.int32, (8, width), 0)
        tail = jnp.where(rows == 3, (norms - target) / n_tokens, 0.0)
        for j, a in enumerate((b_acc, g_acc, o_acc)):
            tail = jnp.where(rows == j, jnp.sum(a[...], axis=0, keepdims=True), tail)
        sums_ref[width:, :] = tail


def head_grad(du0, du1, pre, z, w, gain, lse, n_own, n_tokens):
    slots, width = pre.shape
    block = slots // 2
    part = pl.BlockSpec((block, width), lambda i: (i, 0))
    whole = lambda a: pl.BlockSpec(a, lambda i: (0, 0), pipeline_mode=pl.Buffered(1))
    return pl.pallas_call(
        functools.partial(head_grad_kernel, n_own, n_tokens),
        name="head_grad",
        grid=(2,),
        in_specs=[part, part, part, part, whole((width, width)), whole((1, width)), whole((slots, 1))],
        out_specs=[whole((width + 8, width)), part],
        out_shape=[jax.ShapeDtypeStruct((width + 8, width), F32), jax.ShapeDtypeStruct((slots, width), BF16)],
        scratch_shapes=[pltpu.VMEM((block, width), BF16)] + [pltpu.VMEM((8, width), F32)] * 3,
        compiler_params=pltpu.CompilerParams(vmem_limit_bytes=55_000_000),
        cost_estimate=pl.CostEstimate(flops=8 * slots * width * width, bytes_accessed=slots * width * 18, transcendentals=slots * width),
    )(du0, du1, pre, z, w, gain.reshape(1, width), lse)


def window_rows(n_masks):
    return -(-(n_masks + SUBLANES - 1) // SUBLANES) * SUBLANES


def scatter_kernel(n_masks, window, pos_ref, dz_ref, out_ref):
    group, seq_len, _ = out_ref.shape
    for q in range(group):
        row = pl.program_id(0) * group + q
        hit = pos_ref[q] == lax.broadcasted_iota(jnp.int32, (seq_len, window), 0)
        rows = dz_ref[pl.ds(window_start(n_masks, row), window), :]
        out_ref[q] = jnp.dot(hit.astype(F32).astype(BF16), rows, preferred_element_type=F32).astype(BF16)


def scatter(mask_pos, dz, seq_len):
    n_rows, n_masks = mask_pos.shape
    width = dz.shape[1]
    window = window_rows(n_masks)
    lead = [n_masks * c % SUBLANES for c in range(n_rows)]
    pos = jnp.stack([jnp.pad(mask_pos[c], (a, window - n_masks - a), constant_values=-1) for c, a in enumerate(lead)])
    return pl.pallas_call(
        functools.partial(scatter_kernel, n_masks, window),
        name="scatter",
        grid=(n_rows // GROUP,),
        in_specs=[pl.BlockSpec((GROUP, 1, window), lambda c: (c, 0, 0)), pl.BlockSpec(dz.shape, lambda c: (0, 0), pipeline_mode=pl.Buffered(1))],
        out_specs=pl.BlockSpec((GROUP, seq_len, width), lambda c: (c, 0, 0)),
        out_shape=jax.ShapeDtypeStruct((n_rows, seq_len, width), BF16),
        cost_estimate=pl.CostEstimate(flops=2 * n_rows * seq_len * window * width, bytes_accessed=n_rows * seq_len * width * 2, transcendentals=0),
    )(pos[:, None, :], dz)


def emb_grad_kernel(tc, n, tail, inv_n, bv, grid_tiles, mode, *refs):
    off_ref, lab_ref, lse_ref, emb_ref, bias_ref, u_hbm, *rest = refs
    if mode == "first":
        out_ref, u_out, u_ref, s0, s1, bb_ref, db_acc, in_sem, stage, out_sem = rest
    elif mode == "place":
        acc, db_ref, full_ref, u_ref, s0, s1, bb_ref, db_acc, in_sem = rest
    else:
        rows1, rows2, _, acc, db_ref, full_ref, u_ref, s0, s1, bb_ref, db_acc, in_sem, cbuf, cin_sem, cout_sem, put_sem = rest
    if mode == "first":
        acc, db_ref = out_ref.at[pl.ds(0, bv), :], out_ref.at[pl.ds(bv, 1), pl.ds(0, bv)]
    step = pl.program_id(0)
    tile = off_ref[0] + step
    row0 = tile * bv
    last = n + (1 if tail else 0)

    def at(i):
        return i * tc if isinstance(i, int) else pl.multiple_of(i * tc, tc)

    def size(i):
        return tail if isinstance(i, int) and i == n else tc

    def fetch(i):
        slot = stage.at[i % 4 if isinstance(i, int) else lax.rem(i, 4)] if mode == "first" else u_ref.at[pl.ds(at(i), size(i)), :]
        if mode == "first" and size(i) != tc:
            slot = slot.at[pl.ds(0, size(i)), :]
        return pltpu.make_async_copy(u_hbm.at[pl.ds(at(i), size(i)), :], slot, in_sem.at[i])

    def hand_on(i):
        here = pl.ds(at(i), size(i))
        return pltpu.make_async_copy(u_ref.at[here, :], u_out.at[here, :], out_sem.at[i])

    def arrive(i):
        fetch(i).wait()

    def rounded(i):
        slot = i % 4 if isinstance(i, int) else lax.rem(i, 4)
        u_ref[pl.ds(at(i), size(i)), :] = stage[slot, : size(i), :].astype(BF16)

    def dot1(i):
        return lax.dot_general(emb_ref[...], u_ref[pl.ds(at(i), size(i)), :], NT, preferred_element_type=F32)

    def grad(s_ref, i):
        ids = row0 + lax.broadcasted_iota(jnp.int32, (bv, LANES), 0)
        total = None
        parts = []
        for j in range(size(i) // LANES):
            cols = pl.ds(at(i) + LANES * j, LANES)
            x = s_ref[:, LANES * j : LANES * (j + 1)] + bb_ref[...] - lse_ref[:, cols]
            g = jnp.exp(x) - jnp.where(ids == lab_ref[:, cols], inv_n, 0.0)
            total = g if total is None else total + g
            parts.append(g.astype(BF16))
        db_acc[...] += total
        return jnp.concatenate(parts, axis=1)

    def dot2(s_ref, i):
        acc[...] += jnp.dot(grad(s_ref, i), u_ref[pl.ds(at(i), size(i)), :], preferred_element_type=F32)

    if mode == "first":
        for i in range(4):
            fetch(i).start()
    else:

        @pl.when(step == 0)
        def _():
            for i in range(last):
                fetch(i).start()

    bb_ref[...] = jnp.broadcast_to(bias_ref[...], (LANES, bv)).T
    db_acc[...] = jnp.zeros_like(db_acc)
    acc[...] = jnp.zeros_like(acc)

    def need(*chunks):
        if mode != "first":

            @pl.when(step == 0)
            def _():
                for i in chunks:
                    arrive(i)

    if mode == "first":
        arrive(0)
        rounded(0)
    need(0)
    s0[...] = dot1(0)
    if mode == "first":
        for i in (1, 2):
            arrive(i)
            rounded(i)
        hand_on(0).start()
        for i in range(3):
            if i + 4 < last:
                fetch(i + 4).start()

    def two_chunks(a):
        if mode == "first":
            for i in (a + 3, a + 4):
                arrive(i)
            for i in (a + 1, a + 2):
                hand_on(i).start()
        elif mode == "finish":
            copy_blocks(step * (n // 2 - 1) + a // 2)
        need(a + 1, a + 2)
        s1[...] = dot1(a + 1)
        dot2(s0, a)
        if mode == "first":
            for i in (a + 3, a + 4):
                rounded(i)
        s0[...] = dot1(a + 2)
        dot2(s1, a + 1)
        if mode == "first":
            for i in (a + 7, a + 8):
                if isinstance(i, int):
                    if i < last:
                        fetch(i).start()
                else:
                    full_chunks = i < n
                    pl.when(full_chunks)(lambda i=i: fetch(i).start())
                    if tail:
                        pl.when(i == n)(lambda: fetch(n).start())

    def copy_blocks(t):
        n1, n2 = rows1.shape[0], rows2.shape[0] // bv
        t = jnp.int32(t)
        slot, other = lax.rem(t, 2), 1 - lax.rem(t, 2)
        put = lambda x, where: pltpu.make_async_copy(cbuf.at[x], full_ref.at[pl.ds(where, bv), :], cout_sem.at[x])
        take1 = lambda x, b: pltpu.make_async_copy(rows1.at[b, pl.ds(0, bv), :], cbuf.at[x], cin_sem.at[x])
        take2 = lambda x, b: pltpu.make_async_copy(rows2.at[pl.ds(pl.multiple_of(b * bv, bv), bv), :], cbuf.at[x], cin_sem.at[x])

        @pl.when((t >= 2) & (t < n1 + n2 + 2))
        def _():
            put(slot, 0).wait()

        @pl.when(t < n1)
        def _():
            take1(slot, t).start()

        @pl.when((t >= n1) & (t < n1 + n2))
        def _():
            take2(slot, t - n1).start()

        @pl.when((t >= 1) & (t < n1 + n2 + 1))
        def _():
            take1(other, 0).wait()
            where = jnp.where(t <= n1, t - 1, off_ref[1] + t - 1 - n1) * bv
            put(other, pl.multiple_of(where, bv)).start()

    def body(i, carry):
        two_chunks(2 * i)
        return carry

    trips = n // 2 - 1
    if mode == "first":
        lax.fori_loop(0, trips - 1, body, 0)
        two_chunks(2 * (trips - 1))
    else:
        lax.fori_loop(0, trips, body, 0)
    if mode == "first":
        for i in range(n - 1, last):
            hand_on(i).start()
    need(*range(n - 1, last))
    s1[...] = dot1(n - 1)
    dot2(s0, n - 2)
    if tail:
        s0[:, :tail] = dot1(n)
    dot2(s1, n - 1)
    if tail:
        dot2(s0, n)

    db_ref[...] = jnp.sum(db_acc[...].T, axis=0, keepdims=True)
    if mode == "first":
        for i in range(last):
            hand_on(i).wait()
    elif mode == "place":
        full_ref[...] = acc[...]
    else:
        rows = full_ref.shape[0]
        whole, part = rows // bv, rows % bv

        def put_tile(which, count):
            place = pl.ds(pl.multiple_of((off_ref[0] + which) * bv, bv), count)
            return pltpu.make_async_copy(acc.at[pl.ds(0, count), :], full_ref.at[place, :], put_sem.at[which])

        final = grid_tiles - 1
        pl.when(step < final)(lambda: put_tile(step, bv).start())

        @pl.when((step == final) & (tile < whole))
        def _():
            put_tile(final, bv).start()

        if part:

            @pl.when((step == final) & (tile == whole))
            def _():
                put_tile(final, part).start()

        @pl.when(step == pl.num_programs(0) - 1)
        def _():
            for t in range(grid_tiles * trips, rows1.shape[0] + rows2.shape[0] // bv + 2):
                copy_blocks(t)
            for which in range(final):
                put_tile(which, bv).wait()

        pl.when((step == final) & (tile < whole))(lambda: put_tile(final, bv).wait())
        if part:
            pl.when((step == final) & (tile == whole))(lambda: put_tile(final, part).wait())


def emb_grad(mode, tiles, n_tiles, inv_n, labels, lse, emb, bias, u, *moved):
    n_tok, width = u.shape
    n, tail = divmod(n_tok, TILE_T)
    if n % 2:
        n, tail = n - 1, tail + TILE_T
    chunks = n + (1 if tail else 0)
    bv = TILE_V
    assert mode != "finish" or n_tiles == 2
    rows = n_tiles * bv
    once = pl.Buffered(1)
    anywhere = pl.BlockSpec(memory_space=pl.ANY)
    full = jax.ShapeDtypeStruct(emb.shape, F32)
    extra = 8 if mode == "first" else 0
    out_specs = [pl.BlockSpec((bv + extra, width), lambda i, o: (i, 0))]
    out_shape = [jax.ShapeDtypeStruct((n_tiles * (bv + extra), width), F32)]
    if mode != "first":
        out_specs.append(pl.BlockSpec((None, 1, bv), lambda i, o: (i, 0, 0)))
        out_shape.append(jax.ShapeDtypeStruct((n_tiles, 1, bv), F32))
    scratch = [
        pltpu.VMEM((n_tok, width), BF16),
        pltpu.VMEM((bv, TILE_T), F32),
        pltpu.VMEM((bv, TILE_T), F32),
        pltpu.VMEM((bv, LANES), F32),
        pltpu.VMEM((bv, LANES), F32),
        pltpu.SemaphoreType.DMA((chunks,)),
    ]
    if mode == "first":
        out_specs.append(anywhere)
        out_shape.append(jax.ShapeDtypeStruct(u.shape, BF16))
        scratch += [pltpu.VMEM((4, TILE_T, width), F32), pltpu.SemaphoreType.DMA((chunks,))]
    elif mode == "place":
        out_specs.append(pl.BlockSpec((bv, width), lambda i, o: (o[0] + i, 0)))
        out_shape.append(full)
    else:
        out_specs.append(anywhere)
        out_shape.append(full)
        scratch += [pltpu.VMEM((2, bv, width), F32), pltpu.SemaphoreType.DMA((2,)), pltpu.SemaphoreType.DMA((2,)), pltpu.SemaphoreType.DMA((n_tiles,))]
    grid_spec = pltpu.PrefetchScalarGridSpec(
        num_scalar_prefetch=1,
        grid=(n_tiles,),
        in_specs=[
            pl.BlockSpec((1, n_tok), lambda i, o: (0, 0), pipeline_mode=once),
            pl.BlockSpec((1, n_tok), lambda i, o: (0, 0), pipeline_mode=once),
            pl.BlockSpec((bv, width), lambda i, o: (o[0] + i, 0)),
            pl.BlockSpec((1, bv), lambda i, o: (0, o[0] + i)),
        ]
        + [anywhere] * (1 + len(moved)),
        out_specs=out_specs,
        scratch_shapes=scratch,
    )
    flops = 4 * rows * n_tok * width
    return pl.pallas_call(
        functools.partial(emb_grad_kernel, TILE_T, n, tail, inv_n, bv, n_tiles, mode),
        grid_spec=grid_spec,
        out_shape=out_shape,
        input_output_aliases={8: 2} if mode == "finish" else {},
        compiler_params=pltpu.CompilerParams(vmem_limit_bytes=62_000_000),
        cost_estimate=pl.CostEstimate(flops=flops, bytes_accessed=n_tok * width * 2 + rows * width * 6, transcendentals=rows * n_tok),
    )(tiles, labels, lse, emb, bias, u, *moved)


def copy_kernel(off_ref, src_ref, full_ref, out_ref):
    out_ref[...] = src_ref[...]


def put_rows(first_tile, src, full, n_src, n_tiles):
    bv, width = TILE_V, full.shape[1]
    return pl.pallas_call(
        copy_kernel,
        grid_spec=pltpu.PrefetchScalarGridSpec(
            num_scalar_prefetch=1,
            grid=(n_src, n_tiles),
            in_specs=[pl.BlockSpec((None, bv, width), lambda d, i, o: (d, i, 0)), pl.BlockSpec(memory_space=pl.ANY)],
            out_specs=pl.BlockSpec((bv, width), lambda d, i, o: (o[0] + d * n_tiles + i, 0)),
        ),
        out_shape=jax.ShapeDtypeStruct(full.shape, full.dtype),
        input_output_aliases={2: 0},
        cost_estimate=pl.CostEstimate(flops=n_src * n_tiles * bv * width, bytes_accessed=n_src * n_tiles * bv * width * 8, transcendentals=0),
    )(first_tile, src, full)


def solution(mesh):
    n_groups, n_vp = mesh.shape["dp"], mesh.shape["vp"]

    def local_step(hidden, mask_pos, labels, w_trans, b_trans, ln_gain, ln_bias, emb_table, b_vocab):
        n_rows, seq_len, width = hidden.shape
        n_masks = mask_pos.shape[1]
        shard_rows = emb_table.shape[0]
        n_own = n_rows * n_masks
        n_tokens = n_own * n_groups
        pad = -n_own % (SUBLANES * n_vp)
        me = lax.axis_index("dp")
        row_start = lax.axis_index("vp") * shard_rows
        vp = lax.axis_index("vp")

        slots = n_own + pad
        half = slots // n_vp
        z, pre_act, u_own, sent = head(vp.reshape(1), mask_pos, hidden, w_trans, b_trans, ln_gain, ln_bias, slots, half)
        gathered = lax.all_gather(sent, ("vp", "dp"), axis=0, tiled=True)

        def token_order(rows):
            return jnp.swapaxes(rows.reshape(n_groups, n_vp, half), 0, 1).reshape(1, -1)

        logits, top, total = own_stats(u_own, emb_table, b_vocab)
        label_row = jnp.pad(labels.reshape(1, n_own).astype(F32), ((0, 0), (0, pad)), constant_values=-1.0)
        stats = jnp.concatenate([jnp.concatenate([top, total], axis=1).T, label_row])
        stats = jnp.pad(stats, ((0, 0), (0, -slots % 1024))).reshape(-1, LANES)
        stats = lax.all_gather(stats, ("vp", "dp"), axis=0, tiled=True).reshape(n_vp, n_groups, 3, -1)
        labels_all = token_order(stats[0, :, 2, :slots].astype(jnp.int32) - row_start)
        top = jnp.max(stats[:, :, 0], axis=0)
        log_norm = top + jnp.log(jnp.sum(stats[:, :, 1] * jnp.exp(stats[:, :, 0] - top), axis=0))
        lse = jnp.where(jnp.arange(log_norm.shape[1]) < n_own, log_norm + math.log(n_tokens), -NEGATIVE)[:, :slots]
        lse_all = token_order(lse)
        lse_own = lax.dynamic_slice_in_dim(lse, me, 1).reshape(slots, 1)
        label_col = jnp.pad((labels - row_start).reshape(n_own, 1), ((0, pad), (0, 0)), constant_values=-(2**30))
        du_part = own_du(logits, emb_table, lse_own, label_col, 1.0 / n_tokens, n_own)

        tiles = pl.cdiv(shard_rows, TILE_V)
        k = GATHERED_TILES
        m = (tiles - n_groups * k) // 2
        core = lax.rem(me, 2)
        bias_row = b_vocab.reshape(1, shard_rows)
        lse_all, du_part = lax.optimization_barrier((lse_all, du_part))
        pair = lambda a, b: jnp.stack([a, b]).astype(jnp.int32)
        part1, u_all = emb_grad("first", pair(me * k, 0), k, 1.0 / n_tokens, labels_all, lse_all, emb_table, bias_row, gathered)
        du_other = lax.ppermute(du_part, "vp", [(0, 1), (1, 0)])
        rows1 = lax.all_gather(part1, "dp", axis=0)

        swap = [(i, i ^ 1) for i in range(n_groups)]
        mb = FINISH_TILES
        ma = m - mb
        mine = n_groups * k + core * m
        theirs = n_groups * k + (1 - core) * m
        part2a, db2a, full = emb_grad("place", pair(mine, theirs), ma, 1.0 / n_tokens, labels_all, lse_all, emb_table, bias_row, u_all)
        rows2a = lax.ppermute(part2a, "dp", swap)

        du_other, db2a = lax.optimization_barrier((du_other, db2a))
        sum_in, dz = head_grad(du_part, du_other, pre_act, z, w_trans, ln_gain, lse_own, n_own, n_tokens)
        sums = lax.psum(sum_in, "dp")

        d_hidden = scatter(mask_pos, dz, seq_len)
        lse_last, d_hidden = lax.optimization_barrier((lse_all, d_hidden))
        part2b, db2b, full = emb_grad("finish", pair(mine + ma, theirs), mb, 1.0 / n_tokens, labels_all, lse_last, emb_table, bias_row, u_all, rows1, rows2a, full)
        rows2b = lax.ppermute(part2b, "dp", swap)
        db2 = jnp.concatenate([db2a, db2b]).reshape(-1)
        db2_other = lax.ppermute(db2, "dp", swap)
        d_emb_table = put_rows((theirs + ma).reshape(1), rows2b[None], full, 1, mb)
        db1_all = rows1.reshape(n_groups * k, TILE_V + 8, width)[:, TILE_V, :TILE_V].reshape(-1)
        db_first, db_last = jnp.where(core == 0, db2, db2_other), jnp.where(core == 0, db2_other, db2)
        d_b_vocab = jnp.concatenate([db1_all, db_first, db_last])[:shard_rows]
        return sums[width + 3, 0], d_hidden, sums[:width], sums[width], sums[width + 1], sums[width + 2], d_emb_table, d_b_vocab

    in_specs = (P("dp", None, None), P("dp", None), P("dp", None), P(None, None), P(None), P(None), P(None), P("vp", None), P("vp"))
    out_specs = (P(), P("dp", None, None), P(None, None), P(None), P(None), P(None), P("vp", None), P("vp"))

    return jax.shard_map(local_step, mesh=mesh, in_specs=in_specs, out_specs=out_specs, check_vma=False)
```
